32 devices in a mesh: dp: 1 (over z), cp: 32 (over y, x, core).
Axes of the slice: x: 4, y: 4, z: 1, core: 2. Of those that a mesh axis runs over, the one named last changes fastest.
The devices are a block of a 4x4x8 slice.
Arguments:
- hidden: bfloat16 [16384, 4096], P(('dp', 'cp'))
- w_q: bfloat16 [4096, 16, 128], replicated
- w_k: bfloat16 [4096, 4, 128], replicated
- w_v: bfloat16 [4096, 4, 128], replicated
- w_o: bfloat16 [16, 128, 4096], replicated
Outputs:
- output: bfloat16 [16384, 4096], P(('dp', 'cp'))
All inputs are finite; a program needn't handle non-finite values.
Results may differ from the reference program's by a relative error of at most 0.00450576.
Values are sent between devices in bfloat16 or wider.
A program may use at most 768 MiB of HBM per device.

```python
import jax
import jax.numpy as jnp
from jax import lax

CP_SIZE = 32
CHUNK = 256
MODEL_DIM = 4096
HEADS = 16
KV_HEADS = 4
HEAD_DIM = 128
WINDOW = 4096
ROPE_BASE = 10000


def setup_inputs(seed: int = 0, part: int = 0) -> dict:
    seq_len = 2 * CP_SIZE * CHUNK
    weight_keys = jax.random.split(jax.random.key(seed), 4)
    part_key = jax.random.fold_in(jax.random.key(seed + 1), part)
    noise_key, chunk_key = jax.random.split(part_key)
    token_noise = jax.random.normal(noise_key, (2 * CP_SIZE, CHUNK, MODEL_DIM), jnp.float32)
    chunk_means = jax.random.normal(chunk_key, (2 * CP_SIZE, 1, MODEL_DIM), jnp.float32)
    natural = 0.6 * token_noise + 0.8 * chunk_means
    stored = jnp.stack([natural[:CP_SIZE], natural[CP_SIZE:][::-1]], axis=1).reshape(seq_len, MODEL_DIM)
    in_scale = MODEL_DIM ** -0.5
    out_scale = (HEADS * HEAD_DIM) ** -0.5
    w_q = jax.random.normal(weight_keys[0], (MODEL_DIM, HEADS, HEAD_DIM), jnp.float32) * in_scale
    w_k = jax.random.normal(weight_keys[1], (MODEL_DIM, KV_HEADS, HEAD_DIM), jnp.float32) * in_scale
    w_v = jax.random.normal(weight_keys[2], (MODEL_DIM, KV_HEADS, HEAD_DIM), jnp.float32) * in_scale
    w_o = jax.random.normal(weight_keys[3], (HEADS, HEAD_DIM, MODEL_DIM), jnp.float32) * out_scale
    return {'hidden': stored.astype(jnp.bfloat16), 'w_q': w_q.astype(jnp.bfloat16), 'w_k': w_k.astype(jnp.bfloat16), 'w_v': w_v.astype(jnp.bfloat16), 'w_o': w_o.astype(jnp.bfloat16)}


def rotate(values, positions, factor):
    half_dim = values.shape[-1] // 2
    inv_freq = 1.0 / (ROPE_BASE ** (jnp.arange(half_dim, dtype=jnp.float32) * (2.0 / values.shape[-1])))
    angles = positions.astype(jnp.float32)[..., None, None] * inv_freq
    cos_part = jnp.cos(angles)
    sin_part = jnp.sin(angles)
    first_half = values[..., :half_dim].astype(jnp.float32)
    second_half = values[..., half_dim:].astype(jnp.float32)
    rotated = jnp.concatenate([first_half * cos_part - second_half * sin_part, second_half * cos_part + first_half * sin_part], axis=-1)
    return (rotated * factor).astype(jnp.bfloat16)


def to_natural(stored):
    blocks = stored.reshape((CP_SIZE, 2, CHUNK) + stored.shape[1:])
    return jnp.concatenate([blocks[:, 0], blocks[::-1, 1]], axis=0).reshape(stored.shape)


def to_stored(natural):
    blocks = natural.reshape((2 * CP_SIZE, CHUNK) + natural.shape[1:])
    return jnp.stack([blocks[:CP_SIZE], blocks[CP_SIZE:][::-1]], axis=1).reshape(natural.shape)


def reference(hidden, w_q, w_k, w_v, w_o):
    seq_len = hidden.shape[0]
    group_size = HEADS // KV_HEADS
    dev_ids = jnp.arange(CP_SIZE)[:, None]
    chunk_ids = jnp.concatenate([dev_ids, 2 * CP_SIZE - 1 - dev_ids], axis=1)
    positions = (chunk_ids[:, :, None] * CHUNK + jnp.arange(CHUNK)).reshape(seq_len)
    q_flat = jnp.dot(hidden, w_q.reshape(MODEL_DIM, HEADS * HEAD_DIM), preferred_element_type=jnp.float32).astype(jnp.bfloat16)
    k_flat = jnp.dot(hidden, w_k.reshape(MODEL_DIM, KV_HEADS * HEAD_DIM), preferred_element_type=jnp.float32).astype(jnp.bfloat16)
    v_flat = jnp.dot(hidden, w_v.reshape(MODEL_DIM, KV_HEADS * HEAD_DIM), preferred_element_type=jnp.float32).astype(jnp.bfloat16)
    q_nat = to_natural(rotate(q_flat.reshape(seq_len, HEADS, HEAD_DIM), positions, HEAD_DIM ** -0.5))
    k_nat = to_natural(rotate(k_flat.reshape(seq_len, KV_HEADS, HEAD_DIM), positions, 1.0))
    v_nat = to_natural(v_flat.reshape(seq_len, KV_HEADS, HEAD_DIM))
    block_rows = min(CHUNK, 128)
    key_span = WINDOW + block_rows
    pad_zeros = jnp.zeros((WINDOW, KV_HEADS, HEAD_DIM), jnp.bfloat16)
    k_pad = jnp.concatenate([pad_zeros, k_nat], axis=0)
    v_pad = jnp.concatenate([pad_zeros, v_nat], axis=0)

    def one_block(block_id):
        row_start = block_id * block_rows
        q_part = lax.dynamic_slice_in_dim(q_nat, row_start, block_rows, axis=0).reshape(block_rows, KV_HEADS, group_size, HEAD_DIM)
        k_part = lax.dynamic_slice_in_dim(k_pad, row_start, key_span, axis=0)
        v_part = lax.dynamic_slice_in_dim(v_pad, row_start, key_span, axis=0)
        q_pos = row_start + jnp.arange(block_rows)
        k_pos = row_start - WINDOW + jnp.arange(key_span)
        allowed = (k_pos[None, :] <= q_pos[:, None]) & (q_pos[:, None] - k_pos[None, :] < WINDOW) & (k_pos[None, :] >= 0)
        scores = jnp.einsum('qkgd,skd->kgqs', q_part.astype(jnp.float32), k_part.astype(jnp.float32))
        scores = jnp.where(allowed, scores, -jnp.inf)
        row_max = jnp.max(scores, axis=-1, keepdims=True)
        exp_scores = jnp.exp(scores - row_max)
        row_sum = jnp.sum(exp_scores, axis=-1)
        attn_out = jnp.einsum('kgqs,skd->qkgd', exp_scores.astype(jnp.bfloat16).astype(jnp.float32), v_part.astype(jnp.float32))
        attn_out = attn_out / jnp.transpose(row_sum, (2, 0, 1))[..., None]
        return attn_out.astype(jnp.bfloat16).reshape(block_rows, HEADS * HEAD_DIM)

    o_nat = lax.map(one_block, jnp.arange(seq_len // block_rows)).reshape(seq_len, HEADS * HEAD_DIM)
    o_stored = to_stored(o_nat)
    return jnp.dot(o_stored, w_o.reshape(HEADS * HEAD_DIM, MODEL_DIM), preferred_element_type=jnp.float32).astype(jnp.bfloat16)
```

```python
import functools
import math

import jax
import jax.numpy as jnp
from jax import lax
from jax.experimental import pallas as pl
from jax.experimental.pallas import tpu as pltpu
from jax.sharding import PartitionSpec as P

WINDOW = 4096
ROPE_BASE = 10000.0
NEG = -jnp.inf


def rotate(values, positions, factor):
    half_dim = values.shape[-1] // 2
    inv_freq = 1.0 / (ROPE_BASE ** (jnp.arange(half_dim, dtype=jnp.float32) * (2.0 / values.shape[-1])))
    angles = positions.astype(jnp.float32)[..., None, None] * inv_freq
    cos_part = jnp.cos(angles)
    sin_part = jnp.sin(angles)
    first_half = values[..., :half_dim].astype(jnp.float32)
    second_half = values[..., half_dim:].astype(jnp.float32)
    rotated = jnp.concatenate([first_half * cos_part - second_half * sin_part, second_half * cos_part + first_half * sin_part], axis=-1)
    return (rotated * factor).astype(jnp.bfloat16)


class Plan:
    def __init__(self, cp_size):
        self.chips = cp_size // 2
        self.row = math.isqrt(self.chips)
        self.span = 2 * self.row

    def pair(self, chip, side):
        return jnp.where(side == 0, chip, 2 * self.chips - 1 - chip)

    def chip_of(self, pair):
        return jnp.where(pair < self.chips, pair, 2 * self.chips - 1 - pair)

    def side_of(self, pair):
        return jnp.where(pair < self.chips, 0, 1)

    def twin(self, pair, slot):
        same = 2 * self.chip_of(pair) + slot - (2 * self.chips - 1)
        return jnp.where(pair < self.chips, -1, same)


def attention_kernel(plan, q_ref, kv_ref, out_ref, qbuf, kvbuf, acc, m_ref, l_ref, ostage, orecv,
                     loc_sem, pair_send, pair_recv, send_sem, recv_sem):
    me = lax.axis_index('cp')
    chip = me // 2
    core = lax.rem(me, 2)
    other = 1 - core
    row = plan.row
    x = lax.rem(chip, row)
    y = chip // row
    n_row = plan.chips // row
    chunk = qbuf.shape[4]
    heads_j = qbuf.shape[2]
    group = qbuf.shape[3]
    head_dim = qbuf.shape[5]
    half_cols = heads_j * group * head_dim

    def device(target_chip, target_core):
        return {'cp': target_chip * 2 + target_core}

    barrier = pltpu.get_barrier_semaphore()
    pl.semaphore_signal(barrier, inc=1, device_id=device(chip, other), device_id_type=pl.DeviceIdType.MESH)
    for step in range(1, row):
        mate = y * row + lax.rem(x + step, row)
        pl.semaphore_signal(barrier, inc=1, device_id=device(mate, core), device_id_type=pl.DeviceIdType.MESH)
    for dy in (-1, 1):
        @pl.when((y + dy >= 0) & (y + dy < n_row))
        def _():
            pl.semaphore_signal(barrier, inc=1, device_id=device(chip + dy * row, core), device_id_type=pl.DeviceIdType.MESH)
    pl.semaphore_wait(barrier, row + jnp.where(y > 0, 1, 0) + jnp.where(y < n_row - 1, 1, 0))

    partner = device(chip, other)
    pairs = [plan.pair(chip, s) for s in range(2)]
    own_sub = [core, other]

    pair_kv = []
    pair_q = []
    local = []
    for s in range(2):
        pair_kv.append(pltpu.make_async_remote_copy(
            src_ref=kv_ref.at[other, s], dst_ref=kvbuf.at[s, 0, own_sub[s]], send_sem=pair_send.at[s],
            recv_sem=pair_recv.at[s], device_id=partner, device_id_type=pl.DeviceIdType.MESH))
        pair_q.append(pltpu.make_async_remote_copy(
            src_ref=q_ref.at[other, s], dst_ref=qbuf.at[s, own_sub[s]], send_sem=pair_send.at[2 + s],
            recv_sem=pair_recv.at[2 + s], device_id=partner, device_id_type=pl.DeviceIdType.MESH))
        local.append(pltpu.make_async_copy(kv_ref.at[core, s], kvbuf.at[s, 0, own_sub[s]], loc_sem.at[s]))
        local.append(pltpu.make_async_copy(q_ref.at[core, s], qbuf.at[s, own_sub[s]], loc_sem.at[2 + s]))
    for copy in pair_kv + pair_q + local:
        copy.start()

    acc[...] = jnp.zeros_like(acc)
    l_ref[...] = jnp.zeros_like(l_ref)
    m_ref[...] = jnp.full_like(m_ref, NEG)

    def held(side, slot):
        twin = plan.twin(pairs[side], slot)
        return (jnp.where(twin >= 0, 0, side), jnp.where(twin >= 0, twin, slot))

    sent = []

    def send(side, slot, delta, cond):
        node = pairs[side] + delta
        goal = slot + delta
        ok = cond & (node < 2 * plan.chips) & (pairs[side] - slot >= 0) & (plan.twin(node, goal) < 0)
        held_side, held_slot = held(side, slot)
        index = len(sent)
        copy = pltpu.make_async_remote_copy(
            src_ref=kvbuf.at[held_side, held_slot], dst_ref=kvbuf.at[plan.side_of(node), goal],
            send_sem=send_sem.at[index], recv_sem=recv_sem.at[plan.side_of(node), goal],
            device_id=device(plan.chip_of(node), core), device_id_type=pl.DeviceIdType.MESH)
        sent.append((copy, ok))

        @pl.when(ok)
        def _():
            copy.start()

    def arrive(side, slot, extra=True):
        ok = (pairs[side] - slot >= 0) & (plan.twin(pairs[side], slot) < 0) & extra

        @pl.when(ok)
        def _():
            buf = kvbuf.at[side, slot]
            pltpu.make_async_remote_copy(
                src_ref=buf, dst_ref=buf, send_sem=send_sem.at[0], recv_sem=recv_sem.at[side, slot],
                device_id=partner, device_id_type=pl.DeviceIdType.MESH).wait_recv()

    def along(side, step):
        col = lax.rem(pairs[side], row)
        goal = lax.rem(col + step, row)
        return goal - col

    always = jnp.bool_(True)
    for copy in pair_kv:
        copy.wait_recv()
    for copy in local:
        copy.wait()
    for s in range(2):
        send(s, 0, row, always)
        for step in (1, row - 1) + tuple(range(2, row - 1)):
            delta = along(s, step)
            send(s, 0, delta, delta > 0)
    for copy in pair_q:
        copy.wait_recv()

    def block(side, slot_side, slot, j, a, masked, edge):
        k = kvbuf[slot_side, slot, :, 0, j].reshape(2 * chunk, head_dim)
        v = kvbuf[slot_side, slot, :, 1, j].reshape(2 * chunk, head_dim)
        scores = []
        for g in range(group):
            scores.append(lax.dot_general(qbuf[side, a, j, g], k, (((1,), (1,)), ((), ())), preferred_element_type=jnp.float32))
        if masked:
            rows = lax.broadcasted_iota(jnp.int32, (chunk, 2 * chunk), 0) + a * chunk
            cols = lax.broadcasted_iota(jnp.int32, (chunk, 2 * chunk), 1)
            allowed = (cols > rows) if edge else (cols <= rows)
        for g in range(group):
            s = scores[g]
            if masked:
                s = jnp.where(allowed, s, NEG)
            m_old = m_ref[side, a, j, g]
            m_new = jnp.maximum(m_old, jnp.max(s, axis=1, keepdims=True))
            alpha = jnp.exp(m_old - m_new)
            e = jnp.exp(s - jnp.concatenate([m_new] * (2 * chunk // m_new.shape[1]), axis=1))
            part = e[:, :head_dim]
            for b in range(1, 2 * chunk // head_dim):
                part = part + e[:, b * head_dim:(b + 1) * head_dim]
            m_ref[side, a, j, g] = m_new
            l_ref[side, a, j, g] = l_ref[side, a, j, g] * alpha + part
            acc[side, a, j, g] = acc[side, a, j, g] * alpha + jnp.dot(e.astype(jnp.bfloat16), v, preferred_element_type=jnp.float32)

    def sweep(side, slot, masked=False, edge=False):
        slot_side, at = held(side, slot) if isinstance(side, int) else (
            jnp.where(plan.twin(jnp.where(side == 0, pairs[0], pairs[1]), slot) >= 0, 0, side),
            jnp.where(plan.twin(jnp.where(side == 0, pairs[0], pairs[1]), slot) >= 0,
                      plan.twin(jnp.where(side == 0, pairs[0], pairs[1]), slot), slot))
        mine = jnp.where(side == 0, pairs[0], pairs[1])

        @pl.when(mine - slot >= 0)
        def _():
            def body(i, carry):
                block(side, slot_side, at, i // 2, lax.rem(i, 2), masked, edge)
                return carry
            lax.fori_loop(0, heads_j * 2, body, 0)

    lax.fori_loop(0, 2, lambda s, c: (sweep(s, 0, True, False), c)[1], 0)

    def hand_on(side, cond):
        for step in (1, row - 1) + tuple(range(2, row - 1)):
            delta = along(side, step)
            send(side, row, delta, cond & (delta < 0))
        send(side, row, row, cond)

    arrive(0, row)
    hand_on(0, always)
    arrive(1, row)
    single = plan.twin(pairs[1], row) < 0
    hand_on(1, single)
    sweep_full = lambda side, slot: sweep(side, slot)
    n_near = 2 * (row - 1)

    def near(i, carry):
        return carry

    for d in range(1, row):
        for s in range(2):
            arrive(s, d)
            send(s, d, row, always)
    hand_on(1, jnp.logical_not(single))
    def full(i, carry):
        late = i >= 2 * row
        k = jnp.where(late, i - 2 * row, i)
        slot = jnp.where(late, row + 1, 1) + k // 2
        side = lax.rem(k, 2)

        for d in range(row + 1, plan.span):
            for s in range(2):
                @pl.when(i == 2 * (d - 1) + s)
                def _():
                    arrive(s, d)
        sweep(side, slot)
        return carry

    lax.fori_loop(0, 2 * (plan.span - 1), full, 0)
    arrive(0, plan.span)
    arrive(1, plan.span)
    lax.fori_loop(0, 2, lambda s, c: (sweep(s, plan.span, True, True), c)[1], 0)

    first_col = pl.multiple_of(core * half_cols, half_cols)
    back_col = pl.multiple_of(core * half_cols, half_cols)

    def finish(i, carry):
        s = i // 2
        a = lax.rem(i, 2)
        mine = a == jnp.where(s == 0, core, other)
        for j in range(heads_j):
            for g in range(group):
                total = jnp.sum(l_ref[s, a, j, g], axis=1, keepdims=True)
                o = (acc[s, a, j, g] / total).astype(jnp.bfloat16)
                col = (j * group + g) * head_dim
                ostage[jnp.where(mine, 0, 1), s, :, col:col + head_dim] = o
        return carry

    lax.fori_loop(0, 4, finish, 0)
    back = pltpu.make_async_remote_copy(
        src_ref=ostage.at[1], dst_ref=orecv, send_sem=pair_send.at[4], recv_sem=pair_recv.at[4],
        device_id=partner, device_id_type=pl.DeviceIdType.MESH)
    back.start()
    other_col = pl.multiple_of(other * half_cols, half_cols)
    out_ref[:, :, pl.ds(first_col, half_cols)] = ostage[0]
    back.wait_recv()
    out_ref[:, :, pl.ds(other_col, half_cols)] = orecv[...]
    back.wait_send()
    for copy in pair_kv + pair_q:
        copy.wait_send()
    for copy, ok in sent:
        @pl.when(ok)
        def _():
            copy.wait_send()


def attend(plan, q_all, kv_all):
    _, _, heads_j, group, chunk, head_dim = q_all.shape
    bf16, f32 = jnp.bfloat16, jnp.float32
    slots = plan.span + 1
    n_send = 2 * (plan.row + 2 * plan.row + plan.row)
    return pl.pallas_call(
        functools.partial(attention_kernel, plan),
        out_shape=jax.ShapeDtypeStruct((2, chunk, 2 * heads_j * group * head_dim), bf16),
        in_specs=[pl.BlockSpec(memory_space=pltpu.VMEM)] * 2,
        out_specs=pl.BlockSpec(memory_space=pltpu.VMEM),
        scratch_shapes=[
            pltpu.VMEM((2, 2, heads_j, group, chunk, head_dim), bf16),
            pltpu.VMEM((2, slots, 2, 2, heads_j, chunk, head_dim), bf16),
            pltpu.VMEM((2, 2, heads_j, group, chunk, head_dim), f32),
            pltpu.VMEM((2, 2, heads_j, group, chunk, head_dim), f32),
            pltpu.VMEM((2, 2, heads_j, group, chunk, head_dim), f32),
            pltpu.VMEM((2, 2, chunk, heads_j * group * head_dim), bf16),
            pltpu.VMEM((2, chunk, heads_j * group * head_dim), bf16),
            pltpu.SemaphoreType.DMA((4,)),
            pltpu.SemaphoreType.DMA((5,)),
            pltpu.SemaphoreType.DMA((5,)),
            pltpu.SemaphoreType.DMA((64,)),
            pltpu.SemaphoreType.DMA((2, slots)),
        ],
        compiler_params=pltpu.CompilerParams(collective_id=0, has_side_effects=True, vmem_limit_bytes=56 * 1024 * 1024),
        name='attend',
    )(q_all, kv_all)


def solution(mesh):
    cp_size = mesh.shape['cp']
    plan = Plan(cp_size)

    def device_step(hidden, w_q, w_k, w_v, w_o):
        my_index = lax.axis_index('cp')
        chunk_len = hidden.shape[0] // 2
        model_dim = hidden.shape[1]
        heads, head_dim = w_q.shape[1], w_q.shape[2]
        kv_heads = w_k.shape[1]
        group_size = heads // kv_heads
        x_halves = hidden.reshape(2, chunk_len, model_dim)
        chunk_ids = jnp.stack([my_index, 2 * cp_size - 1 - my_index])
        positions = chunk_ids[:, None] * chunk_len + jnp.arange(chunk_len)[None, :]
        key_proj = jnp.einsum('nqd,dhe->nqhe', x_halves, w_k, preferred_element_type=jnp.float32).astype(jnp.bfloat16)
        val_proj = jnp.einsum('nqd,dhe->nqhe', x_halves, w_v, preferred_element_type=jnp.float32).astype(jnp.bfloat16)
        kv = jnp.stack([rotate(key_proj, positions, 1.0), val_proj], axis=1)
        kv_all = kv.reshape(2, 2, chunk_len, 2, kv_heads // 2, head_dim).transpose(3, 0, 1, 4, 2, 5)
        q_proj = jnp.einsum('nqd,dhe->nqhe', x_halves, w_q, preferred_element_type=jnp.float32).astype(jnp.bfloat16)
        queries = rotate(q_proj, positions, head_dim ** -0.5)
        q_all = queries.reshape(2, chunk_len, 2, kv_heads // 2, group_size, head_dim).transpose(2, 0, 3, 4, 1, 5)
        attended = attend(plan, q_all, kv_all)
        out_rows = jnp.dot(attended.reshape(2 * chunk_len, heads * head_dim), w_o.reshape(heads * head_dim, model_dim), preferred_element_type=jnp.float32)
        return out_rows.astype(jnp.bfloat16)

    return jax.shard_map(device_step, mesh=mesh, in_specs=(P(('dp', 'cp'), None), P(), P(), P(), P()), out_specs=P(('dp', 'cp'), None), check_vma=False)
```

```python
import functools
import math

import jax
import jax.numpy as jnp
from jax import lax
from jax.experimental import pallas as pl
from jax.experimental.pallas import tpu as pltpu
from jax.sharding import PartitionSpec as P

WINDOW = 4096
ROPE_BASE = 10000.0
NEG = -jnp.inf


def rotary_tables(positions, head_dim):
    half_dim = head_dim // 2
    inv_freq = 1.0 / (ROPE_BASE ** (jnp.arange(half_dim, dtype=jnp.float32) * (2.0 / head_dim)))
    angles = positions.astype(jnp.float32)[:, None] * inv_freq
    cos_part = jnp.cos(angles)
    sin_part = jnp.sin(angles)
    return jnp.concatenate([cos_part, cos_part], axis=-1), jnp.concatenate([-sin_part, sin_part], axis=-1)


def spread(n_heads, size):
    per = size // n_heads
    to = lax.broadcasted_iota(jnp.int32, (size, size), 0)
    of = lax.broadcasted_iota(jnp.int32, (size, size), 1)
    return jnp.where((to % per) * n_heads + to // per == of, 1.0, 0.0).astype(jnp.bfloat16)


def by_head(mix, rows_ref, start, dst_ref, n_heads):
    size = mix.shape[0]
    per = size // n_heads
    wide = jnp.concatenate([rows_ref[pl.ds(start, size)], rows_ref[pl.ds(pl.multiple_of(start + size, size), size)]], axis=1)
    head_dim = wide.shape[1] // 2
    out = jnp.dot(mix, wide, preferred_element_type=jnp.float32).astype(jnp.bfloat16)
    at = pl.multiple_of(start // n_heads, 2 * per)
    for b in range(2):
        for h in range(n_heads):
            dst_ref[pl.ds(pl.multiple_of(at + b * per, per), per), h * head_dim:(h + 1) * head_dim] = out[h * per:(h + 1) * per, b * head_dim:(b + 1) * head_dim]


MIX = 256


def kv_kernel(n_heads, x_ref, wk_ref, wv_ref, cos_ref, sin_ref, out_ref, mix, wk, wv, acc_k, acc_v):
    step = pl.program_id(0)

    @pl.when(step == 0)
    def _():
        mix[...] = spread(n_heads, MIX)
        acc_k[...] = jnp.zeros_like(acc_k)
        acc_v[...] = jnp.zeros_like(acc_v)

    def arrange(i, carry):
        start = pl.multiple_of(i * (2 * MIX), 2 * MIX)
        by_head(mix[...], wk_ref, start, wk, n_heads)
        by_head(mix[...], wv_ref, start, wv, n_heads)
        return carry

    lax.fori_loop(0, wk_ref.shape[0] // (2 * MIX), arrange, 0, unroll=2)
    acc_k[...] += jnp.dot(x_ref[...], wk[...], preferred_element_type=jnp.float32)
    acc_v[...] += jnp.dot(x_ref[...], wv[...], preferred_element_type=jnp.float32)

    @pl.when(step == pl.num_programs(0) - 1)
    def _():
        chunk, head_dim = out_ref.shape[4], out_ref.shape[5]
        half = n_heads // 2
        for n in range(2):
            rows = slice(n * chunk, (n + 1) * chunk)
            for h in range(n_heads):
                cols = slice(h * head_dim, (h + 1) * head_dim)
                k = acc_k[rows, cols].astype(jnp.bfloat16).astype(jnp.float32)
                k = k * cos_ref[rows] + pltpu.roll(k, head_dim // 2, 1) * sin_ref[rows]
                out_ref[h // half, n, 0, h % half] = k.astype(jnp.bfloat16)
                out_ref[h // half, n, 1, h % half] = acc_v[rows, cols].astype(jnp.bfloat16)


def project_kv(hidden, w_k, w_v, cos, sin):
    rows, model_dim = hidden.shape
    n_heads, head_dim = w_k.shape[1:]
    chunk = rows // 2
    depth = model_dim // 4
    bf16, f32 = jnp.bfloat16, jnp.float32
    cols = n_heads * head_dim
    return pl.pallas_call(
        functools.partial(kv_kernel, n_heads),
        grid=(model_dim // depth,),
        in_specs=[
            pl.BlockSpec((rows, depth), lambda i: (0, i)),
            pl.BlockSpec((depth * n_heads, head_dim), lambda i: (i, 0)),
            pl.BlockSpec((depth * n_heads, head_dim), lambda i: (i, 0)),
            pl.BlockSpec((rows, head_dim), lambda i: (0, 0)),
            pl.BlockSpec((rows, head_dim), lambda i: (0, 0)),
        ],
        out_specs=pl.BlockSpec((2, 2, 2, n_heads // 2, chunk, head_dim), lambda i: (0, 0, 0, 0, 0, 0)),
        out_shape=jax.ShapeDtypeStruct((2, 2, 2, n_heads // 2, chunk, head_dim), bf16),
        scratch_shapes=[
            pltpu.VMEM((MIX, MIX), bf16),
            pltpu.VMEM((depth, cols), bf16),
            pltpu.VMEM((depth, cols), bf16),
            pltpu.VMEM((rows, cols), f32),
            pltpu.VMEM((rows, cols), f32),
        ],
        compiler_params=pltpu.CompilerParams(dimension_semantics=('arbitrary',), vmem_limit_bytes=40 * 1024 * 1024),
        name='project_kv',
    )(hidden, w_k.reshape(model_dim * n_heads, head_dim), w_v.reshape(model_dim * n_heads, head_dim), cos, sin)


class Plan:
    def __init__(self, cp_size):
        self.chips = cp_size // 2
        self.row = math.isqrt(self.chips)
        self.span = 2 * self.row

    def pair(self, chip, side):
        return jnp.where(side == 0, chip, 2 * self.chips - 1 - chip)

    def chip_of(self, pair):
        return jnp.where(pair < self.chips, pair, 2 * self.chips - 1 - pair)

    def side_of(self, pair):
        return jnp.where(pair < self.chips, 0, 1)

    def twin(self, pair, slot):
        same = 2 * self.chip_of(pair) + slot - (2 * self.chips - 1)
        return jnp.where(pair < self.chips, -1, same)


def attention_kernel(plan, x_ref, wq_ref, cos_ref, sin_ref, kv_ref, out_ref, qbuf, qstage, kvbuf, acc, m_ref, l_ref,
                     ostage, orecv, mix, wraw, wsort, accq, loc_sem, w_sem, pair_send, pair_recv, send_sem, recv_sem):
    me = lax.axis_index('cp')
    chip = me // 2
    core = lax.rem(me, 2)
    other = 1 - core
    row = plan.row
    x = lax.rem(chip, row)
    y = chip // row
    n_row = plan.chips // row
    chunk = qbuf.shape[4]
    heads_j = qbuf.shape[2]
    group = qbuf.shape[3]
    head_dim = qbuf.shape[5]
    half_cols = heads_j * group * head_dim

    def device(target_chip, target_core):
        return {'cp': target_chip * 2 + target_core}

    barrier = pltpu.get_barrier_semaphore()
    pl.semaphore_signal(barrier, inc=1, device_id=device(chip, other), device_id_type=pl.DeviceIdType.MESH)
    for step in range(1, row):
        mate = y * row + lax.rem(x + step, row)
        pl.semaphore_signal(barrier, inc=1, device_id=device(mate, core), device_id_type=pl.DeviceIdType.MESH)
    for dy in (-1, 1):
        @pl.when((y + dy >= 0) & (y + dy < n_row))
        def _():
            pl.semaphore_signal(barrier, inc=1, device_id=device(chip + dy * row, core), device_id_type=pl.DeviceIdType.MESH)
    pl.semaphore_wait(barrier, row + jnp.where(y > 0, 1, 0) + jnp.where(y < n_row - 1, 1, 0))

    partner = device(chip, other)
    pairs = [plan.pair(chip, s) for s in range(2)]
    own_sub = [core, other]

    n_heads = 2 * heads_j * group
    depth = wsort.shape[0]
    raw_rows = depth * n_heads
    n_blocks = wq_ref.shape[0] // raw_rows

    def fetch(block):
        at = pl.multiple_of(block * raw_rows, raw_rows)
        slot = lax.rem(block, 2)
        return pltpu.make_async_copy(wq_ref.at[pl.ds(at, raw_rows)], wraw.at[slot], w_sem.at[slot])

    fetch(0).start()

    pair_kv = []
    pair_q = []
    local = []
    for s in range(2):
        pair_kv.append(pltpu.make_async_remote_copy(
            src_ref=kv_ref.at[other, s], dst_ref=kvbuf.at[s, 0, own_sub[s]], send_sem=pair_send.at[s],
            recv_sem=pair_recv.at[s], device_id=partner, device_id_type=pl.DeviceIdType.MESH))
        pair_q.append(pltpu.make_async_remote_copy(
            src_ref=qstage.at[s], dst_ref=qbuf.at[s, own_sub[s]], send_sem=pair_send.at[2 + s],
            recv_sem=pair_recv.at[2 + s], device_id=partner, device_id_type=pl.DeviceIdType.MESH))
        local.append(pltpu.make_async_copy(kv_ref.at[core, s], kvbuf.at[s, 0, own_sub[s]], loc_sem.at[s]))
    for copy in pair_kv + local:
        copy.start()

    acc[...] = jnp.zeros_like(acc)
    l_ref[...] = jnp.zeros_like(l_ref)
    m_ref[...] = jnp.full_like(m_ref, NEG)

    def held(side, slot):
        twin = plan.twin(pairs[side], slot)
        return (jnp.where(twin >= 0, 0, side), jnp.where(twin >= 0, twin, slot))

    sent = []

    def along(side, step):
        col = lax.rem(pairs[side], row)
        return lax.rem(col + step, row) - col

    def describe(index, side, slot, where, cond):
        delta = where()
        node = pairs[side] + delta
        goal = slot + delta
        ok = (node < 2 * plan.chips) & (pairs[side] - slot >= 0) & (plan.twin(node, goal) < 0) & cond()
        held_side, held_slot = held(side, slot)
        copy = pltpu.make_async_remote_copy(
            src_ref=kvbuf.at[held_side, held_slot], dst_ref=kvbuf.at[plan.side_of(node), goal],
            send_sem=send_sem.at[index], recv_sem=recv_sem.at[plan.side_of(node), goal],
            device_id=device(plan.chip_of(node), core), device_id_type=pl.DeviceIdType.MESH)
        return copy, ok

    def send(side, slot, where, cond):
        spec = (len(sent), side, slot, where, cond)
        sent.append(spec)
        copy, ok = describe(*spec)

        @pl.when(ok)
        def _():
            copy.start()

    def arrive(side, slot, extra=True):
        ok = (pairs[side] - slot >= 0) & (plan.twin(pairs[side], slot) < 0) & extra

        @pl.when(ok)
        def _():
            buf = kvbuf.at[side, slot]
            pltpu.make_async_remote_copy(
                src_ref=buf, dst_ref=buf, send_sem=send_sem.at[0], recv_sem=recv_sem.at[side, slot],
                device_id=partner, device_id_type=pl.DeviceIdType.MESH).wait_recv()

    def always():
        return pairs[0] >= 0

    def down():
        return row

    for copy in pair_kv:
        copy.wait_recv()
    for copy in local:
        copy.wait()
    for s in range(2):
        send(s, 0, down, always)
    for step in (1, row - 1):
        for s in range(2):
            where = functools.partial(along, s, step)
            send(s, 0, where, lambda w=where: w() > 0)

    mix[...] = spread(n_heads, MIX)
    accq[...] = jnp.zeros_like(accq)

    def project(block, carry):
        fetch(block).wait()

        @pl.when(block + 1 < n_blocks)
        def _():
            fetch(block + 1).start()

        raw = wraw.at[lax.rem(block, 2)]

        def arrange(i, c):
            by_head(mix[...], raw, pl.multiple_of(i * (2 * MIX), 2 * MIX), wsort, n_heads)
            return c

        lax.fori_loop(0, raw_rows // (2 * MIX), arrange, 0, unroll=4)
        at = pl.multiple_of(block * depth, depth)
        accq[...] += jnp.dot(x_ref[:, pl.ds(at, depth)], wsort[...], preferred_element_type=jnp.float32)
        return carry

    lax.fori_loop(0, n_blocks, project, 0)

    def turn(s, half, put):
        rows = pl.ds(pl.multiple_of(s * chunk, chunk), chunk)
        for j in range(heads_j):
            for g in range(group):
                col = pl.multiple_of(half * half_cols, half_cols) + (j * group + g) * head_dim
                q = accq[rows, pl.ds(pl.multiple_of(col, head_dim), head_dim)].astype(jnp.bfloat16).astype(jnp.float32)
                q = q * cos_ref[rows] + pltpu.roll(q, head_dim // 2, 1) * sin_ref[rows]
                put(j, g, (q * head_dim ** -0.5).astype(jnp.bfloat16))

    def for_partner(s, carry):
        def put(j, g, q):
            qstage[s, j, g] = q
        turn(s, other, put)
        return carry

    def for_me(s, carry):
        def put(j, g, q):
            qbuf[s, jnp.where(s == 0, core, other), j, g] = q
        turn(s, core, put)
        return carry

    lax.fori_loop(0, 2, for_partner, 0)
    lax.fori_loop(0, 2, for_me, 0)
    for copy in pair_q:
        copy.start()
    for copy in pair_q:
        copy.wait_recv()

    def block(side, slot_side, slot, j, a, masked, edge):
        k = kvbuf[slot_side, slot, :, 0, j].reshape(2 * chunk, head_dim)
        v = kvbuf[slot_side, slot, :, 1, j].reshape(2 * chunk, head_dim)
        scores = []
        for g in range(group):
            scores.append(lax.dot_general(qbuf[side, a, j, g], k, (((1,), (1,)), ((), ())), preferred_element_type=jnp.float32))
        if masked:
            rows = lax.broadcasted_iota(jnp.int32, (chunk, 2 * chunk), 0) + a * chunk
            cols = lax.broadcasted_iota(jnp.int32, (chunk, 2 * chunk), 1)
            allowed = (cols > rows) if edge else (cols <= rows)
        for g in range(group):
            s = scores[g]
            if masked:
                s = jnp.where(allowed, s, NEG)
            m_old = m_ref[side, a, j, g]
            m_new = jnp.maximum(m_old, jnp.max(s, axis=1, keepdims=True))
            alpha = jnp.exp(m_old - m_new)
            e = jnp.exp(s - jnp.concatenate([m_new] * (2 * chunk // m_new.shape[1]), axis=1))
            part = e[:, :head_dim]
            for b in range(1, 2 * chunk // head_dim):
                part = part + e[:, b * head_dim:(b + 1) * head_dim]
            m_ref[side, a, j, g] = m_new
            l_ref[side, a, j, g] = l_ref[side, a, j, g] * alpha + part
            acc[side, a, j, g] = acc[side, a, j, g] * alpha + jnp.dot(e.astype(jnp.bfloat16), v, preferred_element_type=jnp.float32)

    def sweep(side, slot, masked=False, edge=False):
        slot_side, at = held(side, slot) if isinstance(side, int) else (
            jnp.where(plan.twin(jnp.where(side == 0, pairs[0], pairs[1]), slot) >= 0, 0, side),
            jnp.where(plan.twin(jnp.where(side == 0, pairs[0], pairs[1]), slot) >= 0,
                      plan.twin(jnp.where(side == 0, pairs[0], pairs[1]), slot), slot))
        mine = jnp.where(side == 0, pairs[0], pairs[1])

        @pl.when(mine - slot >= 0)
        def _():
            def body(i, carry):
                block(side, slot_side, at, i // 2, lax.rem(i, 2), masked, edge)
                return carry
            lax.fori_loop(0, heads_j * 2, body, 0)

    lax.fori_loop(0, 2, lambda s, c: (sweep(s, 0, True, False), c)[1], 0)

    def hand_on(side, cond):
        for step in (1, row - 1):
            where = functools.partial(along, side, step)
            send(side, row, where, lambda w=where: cond() & (w() < 0))
        send(side, row, down, cond)

    def single():
        return plan.twin(pairs[1], row) < 0

    def double():
        return plan.twin(pairs[1], row) >= 0

    near, far = 1, row - 1

    def pass_on(side, slot):
        def inner():
            col = lax.rem(pairs[side], row)
            return (col > 0) & (col < row - 1)

        send(side, slot, down, always)
        if slot == near:
            send(side, slot, lambda: 1, inner)
        if slot == far:
            send(side, slot, lambda: -1, inner)

    def come(side, slot):
        def event():
            arrive(side, slot)
            if slot < row:
                pass_on(side, slot)
        return event

    def first():
        arrive(0, row)
        hand_on(0, always)
        arrive(1, row)
        hand_on(1, single)

    order = [
        (0, 4, first), (0, 1, come(0, 1)), (1, 1, come(1, 1)), (0, 3, come(0, 3)), (0, 2, come(0, 2)), (1, 3, come(1, 3)),
        (1, 2, come(1, 2)), (1, 4, lambda: hand_on(1, double)),
        (0, 8, come(0, 8)), (0, 5, come(0, 5)), (1, 5, come(1, 5)), (0, 7, come(0, 7)), (1, 8, come(1, 8)),
        (0, 6, come(0, 6)), (1, 6, come(1, 6)), (1, 7, come(1, 7)),
    ]

    def visit(i, carry):
        side = jnp.int32(0)
        slot = jnp.int32(0)
        for n, (s, d, event) in enumerate(order):
            side = jnp.where(i == n, s, side)
            slot = jnp.where(i == n, d, slot)

            @pl.when(i == n)
            def _():
                event()

        @pl.when(slot < plan.span)
        def _():
            sweep(side, slot)

        @pl.when(slot == plan.span)
        def _():
            sweep(side, slot, True, True)
        return carry

    lax.fori_loop(0, len(order), visit, 0)

    first_col = pl.multiple_of(core * half_cols, half_cols)
    back_col = pl.multiple_of(core * half_cols, half_cols)

    def finish(i, carry):
        s = i // 2
        a = lax.rem(i, 2)
        mine = a == jnp.where(s == 0, core, other)
        for j in range(heads_j):
            for g in range(group):
                total = jnp.sum(l_ref[s, a, j, g], axis=1, keepdims=True)
                o = (acc[s, a, j, g] / total).astype(jnp.bfloat16)
                col = (j * group + g) * head_dim
                ostage[jnp.where(mine, 0, 1), s, :, col:col + head_dim] = o
        return carry

    lax.fori_loop(0, 4, finish, 0)
    back = pltpu.make_async_remote_copy(
        src_ref=ostage.at[1], dst_ref=orecv, send_sem=pair_send.at[4], recv_sem=pair_recv.at[4],
        device_id=partner, device_id_type=pl.DeviceIdType.MESH)
    back.start()
    other_col = pl.multiple_of(other * half_cols, half_cols)
    out_ref[:, :, pl.ds(first_col, half_cols)] = ostage[0]
    back.wait_recv()
    out_ref[:, :, pl.ds(other_col, half_cols)] = orecv[...]
    back.wait_send()
    for copy in pair_kv + pair_q:
        copy.wait_send()
    for spec in sent:
        copy, ok = describe(*spec)

        @pl.when(ok)
        def _():
            copy.wait_send()


def attend(plan, hidden, w_q, cos, sin, kv_all):
    model_dim, heads, head_dim = w_q.shape
    _, _, _, heads_j, chunk, _ = kv_all.shape
    group = heads // (2 * heads_j)
    bf16, f32 = jnp.bfloat16, jnp.float32
    slots = plan.span + 1
    depth = model_dim // 8
    vmem = pl.BlockSpec(memory_space=pltpu.VMEM)
    return pl.pallas_call(
        functools.partial(attention_kernel, plan),
        out_shape=jax.ShapeDtypeStruct((2, chunk, heads * head_dim), bf16),
        in_specs=[vmem, pl.BlockSpec(memory_space=pl.ANY), vmem, vmem, vmem],
        out_specs=vmem,
        scratch_shapes=[
            pltpu.VMEM((2, 2, heads_j, group, chunk, head_dim), bf16),
            pltpu.VMEM((2, heads_j, group, chunk, head_dim), bf16),
            pltpu.VMEM((2, slots, 2, 2, heads_j, chunk, head_dim), bf16),
            pltpu.VMEM((2, 2, heads_j, group, chunk, head_dim), f32),
            pltpu.VMEM((2, 2, heads_j, group, chunk, head_dim), f32),
            pltpu.VMEM((2, 2, heads_j, group, chunk, head_dim), f32),
            pltpu.VMEM((2, 2, chunk, heads_j * group * head_dim), bf16),
            pltpu.VMEM((2, chunk, heads_j * group * head_dim), bf16),
            pltpu.VMEM((MIX, MIX), bf16),
            pltpu.VMEM((2, depth * heads, head_dim), bf16),
            pltpu.VMEM((depth, heads * head_dim), bf16),
            pltpu.VMEM((2 * chunk, heads * head_dim), f32),
            pltpu.SemaphoreType.DMA((2,)),
            pltpu.SemaphoreType.DMA((2,)),
            pltpu.SemaphoreType.DMA((5,)),
            pltpu.SemaphoreType.DMA((5,)),
            pltpu.SemaphoreType.DMA((64,)),
            pltpu.SemaphoreType.DMA((2, slots)),
        ],
        compiler_params=pltpu.CompilerParams(collective_id=0, has_side_effects=True, vmem_limit_bytes=60 * 1024 * 1024),
        name='attend',
    )(hidden, w_q.reshape(model_dim * heads, head_dim), cos, sin, kv_all)


def solution(mesh):
    cp_size = mesh.shape['cp']
    plan = Plan(cp_size)

    def device_step(hidden, w_q, w_k, w_v, w_o):
        my_index = lax.axis_index('cp')
        chunk_len = hidden.shape[0] // 2
        model_dim = hidden.shape[1]
        heads, head_dim = w_q.shape[1], w_q.shape[2]
        chunk_ids = jnp.stack([my_index, 2 * cp_size - 1 - my_index])
        positions = (chunk_ids[:, None] * chunk_len + jnp.arange(chunk_len)[None, :]).reshape(2 * chunk_len)
        cos, sin = rotary_tables(positions, head_dim)
        kv_all = project_kv(hidden, w_k, w_v, cos, sin)
        attended = attend(plan, hidden, w_q, cos, sin, kv_all)
        out_rows = jnp.dot(attended.reshape(2 * chunk_len, heads * head_dim), w_o.reshape(heads * head_dim, model_dim), preferred_element_type=jnp.float32)
        return out_rows.astype(jnp.bfloat16)

    return jax.shard_map(device_step, mesh=mesh, in_specs=(P(('dp', 'cp'), None), P(), P(), P(), P()), out_specs=P(('dp', 'cp'), None), check_vma=False)
```

```python
import functools
import math

import jax
import jax.numpy as jnp
from jax import lax
from jax.experimental import pallas as pl
from jax.experimental.pallas import tpu as pltpu
from jax.sharding import PartitionSpec as P

WINDOW = 4096
ROPE_BASE = 10000.0
NEG = -jnp.inf


def rotary_tables(positions, head_dim):
    half_dim = head_dim // 2
    inv_freq = 1.0 / (ROPE_BASE ** (jnp.arange(half_dim, dtype=jnp.float32) * (2.0 / head_dim)))
    angles = positions.astype(jnp.float32)[:, None] * inv_freq
    cos_part = jnp.cos(angles)
    sin_part = jnp.sin(angles)
    return jnp.concatenate([cos_part, cos_part], axis=-1), jnp.concatenate([-sin_part, sin_part], axis=-1)


def spread(n_heads, size):
    per = size // n_heads
    to = lax.broadcasted_iota(jnp.int32, (size, size), 0)
    of = lax.broadcasted_iota(jnp.int32, (size, size), 1)
    return jnp.where((to % per) * n_heads + to // per == of, 1.0, 0.0).astype(jnp.bfloat16)


def by_head(mix, rows_ref, start, dst_ref, n_heads):
    size = mix.shape[0]
    per = size // n_heads
    if len(rows_ref.shape) == 3:
        first = pl.multiple_of(start // n_heads, 2 * per)
        pair = rows_ref[pl.ds(first, 2 * per)].reshape(2 * size, rows_ref.shape[2])
        wide = jnp.concatenate([pair[:size], pair[size:]], axis=1)
    else:
        wide = jnp.concatenate([rows_ref[pl.ds(start, size)], rows_ref[pl.ds(pl.multiple_of(start + size, size), size)]], axis=1)
    head_dim = wide.shape[1] // 2
    out = jnp.dot(mix, wide, preferred_element_type=jnp.float32).astype(jnp.bfloat16)
    at = pl.multiple_of(start // n_heads, 2 * per)
    for b in range(2):
        for h in range(n_heads):
            dst_ref[pl.ds(pl.multiple_of(at + b * per, per), per), h * head_dim:(h + 1) * head_dim] = out[h * per:(h + 1) * per, b * head_dim:(b + 1) * head_dim]


MIX = 256


def kv_kernel(n_heads, x_ref, wk_ref, wv_ref, cos_ref, sin_ref, out_ref, mix, wk, wv, acc_k, acc_v):
    step = pl.program_id(0)

    @pl.when(step == 0)
    def _():
        mix[...] = spread(n_heads, MIX)
        acc_k[...] = jnp.zeros_like(acc_k)
        acc_v[...] = jnp.zeros_like(acc_v)

    def arrange(i, carry):
        start = pl.multiple_of(i * (2 * MIX), 2 * MIX)
        by_head(mix[...], wk_ref, start, wk, n_heads)
        by_head(mix[...], wv_ref, start, wv, n_heads)
        return carry

    lax.fori_loop(0, wk_ref.shape[0] // (2 * MIX), arrange, 0, unroll=4)
    acc_k[...] += jnp.dot(x_ref[...], wk[...], preferred_element_type=jnp.float32)
    acc_v[...] += jnp.dot(x_ref[...], wv[...], preferred_element_type=jnp.float32)

    @pl.when(step == pl.num_programs(0) - 1)
    def _():
        chunk, head_dim = out_ref.shape[4], out_ref.shape[5]
        half = n_heads // 2
        for n in range(2):
            rows = slice(n * chunk, (n + 1) * chunk)
            for h in range(n_heads):
                cols = slice(h * head_dim, (h + 1) * head_dim)
                k = acc_k[rows, cols].astype(jnp.bfloat16).astype(jnp.float32)
                k = k * cos_ref[rows] + pltpu.roll(k, head_dim // 2, 1) * sin_ref[rows]
                out_ref[h // half, n, 0, h % half] = k.astype(jnp.bfloat16)
                out_ref[h // half, n, 1, h % half] = acc_v[rows, cols].astype(jnp.bfloat16)


def project_kv(hidden, w_k, w_v, cos, sin):
    rows, model_dim = hidden.shape
    n_heads, head_dim = w_k.shape[1:]
    chunk = rows // 2
    depth = model_dim // 4
    bf16, f32 = jnp.bfloat16, jnp.float32
    cols = n_heads * head_dim
    return pl.pallas_call(
        functools.partial(kv_kernel, n_heads),
        grid=(model_dim // depth,),
        in_specs=[
            pl.BlockSpec((rows, depth), lambda i: (0, i)),
            pl.BlockSpec((depth * n_heads, head_dim), lambda i: (i, 0)),
            pl.BlockSpec((depth * n_heads, head_dim), lambda i: (i, 0)),
            pl.BlockSpec((rows, head_dim), lambda i: (0, 0)),
            pl.BlockSpec((rows, head_dim), lambda i: (0, 0)),
        ],
        out_specs=pl.BlockSpec((2, 2, 2, n_heads // 2, chunk, head_dim), lambda i: (0, 0, 0, 0, 0, 0)),
        out_shape=jax.ShapeDtypeStruct((2, 2, 2, n_heads // 2, chunk, head_dim), bf16),
        scratch_shapes=[
            pltpu.VMEM((MIX, MIX), bf16),
            pltpu.VMEM((depth, cols), bf16),
            pltpu.VMEM((depth, cols), bf16),
            pltpu.VMEM((rows, cols), f32),
            pltpu.VMEM((rows, cols), f32),
        ],
        compiler_params=pltpu.CompilerParams(dimension_semantics=('arbitrary',), vmem_limit_bytes=62 * 1024 * 1024),
        name='project_kv',
    )(hidden, w_k.reshape(model_dim * n_heads, head_dim), w_v.reshape(model_dim * n_heads, head_dim), cos, sin)


class Plan:
    def __init__(self, cp_size):
        self.chips = cp_size // 2
        self.row = math.isqrt(self.chips)
        self.span = 2 * self.row

    def pair(self, chip, side):
        return jnp.where(side == 0, chip, 2 * self.chips - 1 - chip)

    def chip_of(self, pair):
        return jnp.where(pair < self.chips, pair, 2 * self.chips - 1 - pair)

    def side_of(self, pair):
        return jnp.where(pair < self.chips, 0, 1)

    def twin(self, pair, slot):
        same = 2 * self.chip_of(pair) + slot - (2 * self.chips - 1)
        return jnp.where(pair < self.chips, -1, same)


def attention_kernel(plan, x_hbm, wq_ref, cos_ref, sin_ref, kv_ref, out_ref, qbuf, qstage, kvbuf, acc, m_ref, l_ref,
                     ostage, orecv, x_ref, mix, wraw, wsort, accq, loc_sem, x_sem, w_sem, pair_send, pair_recv, send_sem, recv_sem):
    me = lax.axis_index('cp')
    chip = me // 2
    core = lax.rem(me, 2)
    other = 1 - core
    row = plan.row
    x = lax.rem(chip, row)
    y = chip // row
    n_row = plan.chips // row
    chunk = qbuf.shape[4]
    heads_j = qbuf.shape[2]
    group = qbuf.shape[3]
    head_dim = qbuf.shape[5]
    half_cols = heads_j * group * head_dim

    def device(target_chip, target_core):
        return {'cp': target_chip * 2 + target_core}

    barrier = pltpu.get_barrier_semaphore()
    pl.semaphore_signal(barrier, inc=1, device_id=device(chip, other), device_id_type=pl.DeviceIdType.MESH)
    for step in range(1, row):
        mate = y * row + lax.rem(x + step, row)
        pl.semaphore_signal(barrier, inc=1, device_id=device(mate, core), device_id_type=pl.DeviceIdType.MESH)
    for dy in (-1, 1):
        @pl.when((y + dy >= 0) & (y + dy < n_row))
        def _():
            pl.semaphore_signal(barrier, inc=1, device_id=device(chip + dy * row, core), device_id_type=pl.DeviceIdType.MESH)
    pl.semaphore_wait(barrier, row + jnp.where(y > 0, 1, 0) + jnp.where(y < n_row - 1, 1, 0))

    partner = device(chip, other)
    pairs = [plan.pair(chip, s) for s in range(2)]
    own_sub = [core, other]

    n_heads = heads_j * group
    depth = wsort.shape[0]
    per_half = wq_ref.shape[0] // depth
    n_blocks = 2 * per_half
    load_x = pltpu.make_async_copy(x_hbm, x_ref, x_sem)
    load_x.start()

    def fetch(block):
        at = pl.multiple_of(lax.rem(block, per_half) * depth, depth)
        half = jnp.where(block < per_half, other, core)
        slot = lax.rem(block, 2)
        return pltpu.make_async_copy(wq_ref.at[pl.ds(at, depth), half], wraw.at[slot], w_sem.at[slot])

    fetch(0).start()

    pair_kv = []
    pair_q = []
    local = []
    for s in range(2):
        pair_kv.append(pltpu.make_async_remote_copy(
            src_ref=kv_ref.at[other, s], dst_ref=kvbuf.at[s, 0, own_sub[s]], send_sem=pair_send.at[s],
            recv_sem=pair_recv.at[s], device_id=partner, device_id_type=pl.DeviceIdType.MESH))
        pair_q.append(pltpu.make_async_remote_copy(
            src_ref=qstage.at[s], dst_ref=qbuf.at[s, own_sub[s]], send_sem=pair_send.at[2 + s],
            recv_sem=pair_recv.at[2 + s], device_id=partner, device_id_type=pl.DeviceIdType.MESH))
        local.append(pltpu.make_async_copy(kv_ref.at[core, s], kvbuf.at[s, 0, own_sub[s]], loc_sem.at[s]))
    for copy in pair_kv + local:
        copy.start()

    acc[...] = jnp.zeros_like(acc)
    l_ref[...] = jnp.zeros_like(l_ref)
    m_ref[...] = jnp.full_like(m_ref, NEG)

    def held(side, slot):
        twin = plan.twin(pairs[side], slot)
        return (jnp.where(twin >= 0, 0, side), jnp.where(twin >= 0, twin, slot))

    sent = []

    def along(side, step):
        col = lax.rem(pairs[side], row)
        return lax.rem(col + step, row) - col

    def describe(index, side, slot, where, cond):
        delta = where()
        node = pairs[side] + delta
        goal = slot + delta
        ok = (node < 2 * plan.chips) & (pairs[side] - slot >= 0) & (plan.twin(node, goal) < 0) & cond()
        held_side, held_slot = held(side, slot)
        copy = pltpu.make_async_remote_copy(
            src_ref=kvbuf.at[held_side, held_slot], dst_ref=kvbuf.at[plan.side_of(node), goal],
            send_sem=send_sem.at[index], recv_sem=recv_sem.at[plan.side_of(node), goal],
            device_id=device(plan.chip_of(node), core), device_id_type=pl.DeviceIdType.MESH)
        return copy, ok

    def send(side, slot, where, cond):
        spec = (len(sent), side, slot, where, cond)
        sent.append(spec)
        copy, ok = describe(*spec)

        @pl.when(ok)
        def _():
            copy.start()

    def arrive(side, slot, extra=True):
        ok = (pairs[side] - slot >= 0) & (plan.twin(pairs[side], slot) < 0) & extra

        @pl.when(ok)
        def _():
            buf = kvbuf.at[side, slot]
            pltpu.make_async_remote_copy(
                src_ref=buf, dst_ref=buf, send_sem=send_sem.at[0], recv_sem=recv_sem.at[side, slot],
                device_id=partner, device_id_type=pl.DeviceIdType.MESH).wait_recv()

    def always():
        return pairs[0] >= 0

    def down():
        return row

    for copy in pair_kv:
        copy.wait_recv()
    for copy in local:
        copy.wait()
    near, far = 1, row - 1

    def col_of(side):
        return lax.rem(pairs[side], row)

    def inner(side):
        return (col_of(side) > 0) & (col_of(side) < row - 1)

    def launch(side, slot, cond):
        send(side, slot, down, cond)
        if slot == 0 or slot == row:
            for step in (1, row - 1):
                where = functools.partial(along, side, step)
                send(side, slot, where, lambda w=where: cond() & ((w() > 0) if slot == 0 else (w() < 0)))
        elif slot == near:
            send(side, slot, lambda: 1, lambda: cond() & inner(side))
        elif slot == far:
            send(side, slot, lambda: -1, lambda: cond() & inner(side))

    def echo(slot):
        def as_high(d):
            return plan.twin(pairs[1], d) == slot
        for d in range(1, row + 1):
            if (d - slot) % 2 == 1 and d > slot:
                send(1, d, down, lambda d=d: as_high(d))

    def event(side, slot):
        arrive(side, slot)
        if side == 0:
            launch(0, slot, always)
            echo(slot)
        else:
            launch(1, slot, lambda: plan.twin(pairs[1], slot) < 0)

    launch(0, 0, always)
    launch(1, 0, always)
    echo(0)

    mix[...] = spread(n_heads, MIX)
    load_x.wait()

    def turn(s, half):
        rows = slice(s * chunk, (s + 1) * chunk)
        for j in range(heads_j):
            for g in range(group):
                col = (j * group + g) * head_dim
                q = accq[rows, col:col + head_dim].astype(jnp.bfloat16).astype(jnp.float32)
                q = q * cos_ref[rows] + pltpu.roll(q, head_dim // 2, 1) * sin_ref[rows]
                q = (q * head_dim ** -0.5).astype(jnp.bfloat16)

                @pl.when(half == 0)
                def _():
                    qstage[s, j, g] = q

                @pl.when(half == 1)
                def _():
                    qbuf[s, own_sub[s], j, g] = q

    wave = (row, near, far, 2)

    def project(block, carry):
        fetch(block).wait()

        @pl.when(block + 1 < n_blocks)
        def _():
            fetch(block + 1).start()

        half = block // per_half
        step = lax.rem(block, per_half)
        raw = wraw.at[lax.rem(block, 2)]

        def arrange(i, c):
            by_head(mix[...], raw, pl.multiple_of(i * (2 * MIX), 2 * MIX), wsort, n_heads)
            return c

        lax.fori_loop(0, depth * n_heads // (2 * MIX), arrange, 0, unroll=8)
        at = pl.multiple_of(step * depth, depth)
        part = jnp.dot(x_ref[:, pl.ds(at, depth)], wsort[...], preferred_element_type=jnp.float32)

        @pl.when(step == 0)
        def _():
            accq[...] = part

        @pl.when(step > 0)
        def _():
            accq[...] += part

        @pl.when(step == per_half - 1)
        def _():
            for s in range(2):
                turn(s, half)

        @pl.when(block == per_half - 1)
        def _():
            for copy in pair_q:
                copy.start()

        @pl.when(block == n_blocks - 3)
        def _():
            event(0, wave[0])
            event(1, wave[0])
        return carry

    lax.fori_loop(0, n_blocks, project, 0)
    for copy in pair_q:
        copy.wait_recv()

    def block(side, slot_side, slot, j, subs, masked, edge):
        k = kvbuf[slot_side, slot, :, 0, j].reshape(2 * chunk, head_dim)
        v = kvbuf[slot_side, slot, :, 1, j].reshape(2 * chunk, head_dim)
        tiles = [(a, g) for a in subs for g in range(group)]

        def score(t):
            a, g = tiles[t]
            return lax.dot_general(qbuf[side, a, j, g], k, (((1,), (1,)), ((), ())), preferred_element_type=jnp.float32)

        def update(t, s):
            a, g = tiles[t]
            if masked:
                rows = lax.broadcasted_iota(jnp.int32, (chunk, 2 * chunk), 0) + a * chunk
                cols = lax.broadcasted_iota(jnp.int32, (chunk, 2 * chunk), 1)
                s = jnp.where((cols > rows) if edge else (cols <= rows), s, NEG)
            m_old = m_ref[side, a, j, g]
            m_new = jnp.maximum(m_old, jnp.max(s, axis=1, keepdims=True))
            alpha = jnp.exp(m_old - m_new)
            e = jnp.exp(s - jnp.concatenate([m_new] * (2 * chunk // m_new.shape[1]), axis=1))
            part = e[:, :head_dim]
            for b in range(1, 2 * chunk // head_dim):
                part = part + e[:, b * head_dim:(b + 1) * head_dim]
            m_ref[side, a, j, g] = m_new
            l_ref[side, a, j, g] = l_ref[side, a, j, g] * alpha + part
            acc[side, a, j, g] = acc[side, a, j, g] * alpha + jnp.dot(e.astype(jnp.bfloat16), v, preferred_element_type=jnp.float32)

        ahead = 2
        scores = [score(t) for t in range(ahead)]
        for t in range(len(tiles)):
            if t + ahead < len(tiles):
                scores.append(score(t + ahead))
            update(t, scores[t])

    def sweep(side, slot, masked=False, edge=False):
        slot_side, at = held(side, slot) if isinstance(side, int) else (
            jnp.where(plan.twin(jnp.where(side == 0, pairs[0], pairs[1]), slot) >= 0, 0, side),
            jnp.where(plan.twin(jnp.where(side == 0, pairs[0], pairs[1]), slot) >= 0,
                      plan.twin(jnp.where(side == 0, pairs[0], pairs[1]), slot), slot))
        mine = jnp.where(side == 0, pairs[0], pairs[1])

        @pl.when(mine - slot >= 0)
        def _():
            def body(i, carry):
                block(side, slot_side, at, i, (0, 1), masked, edge)
                return carry
            lax.fori_loop(0, heads_j, body, 0)

    lax.fori_loop(0, 2, lambda s, c: (sweep(s, 0, True, False), c)[1], 0)

    def finish(s):
        def body(i, carry):
            a = jnp.where(i == 0, 1 - own_sub[s], own_sub[s])
            for j in range(heads_j):
                for g in range(group):
                    total = jnp.sum(l_ref[s, a, j, g], axis=1, keepdims=True)
                    o = (acc[s, a, j, g] / total).astype(jnp.bfloat16)
                    col = (j * group + g) * head_dim
                    ostage[1 - i, s, :, col:col + head_dim] = o
            return carry

        lax.fori_loop(0, 2, body, 0)

    def back(s):
        return pltpu.make_async_remote_copy(
            src_ref=ostage.at[1, s], dst_ref=orecv.at[s], send_sem=pair_send.at[4 + s], recv_sem=pair_recv.at[4 + s],
            device_id=partner, device_id_type=pl.DeviceIdType.MESH)

    def low_done():
        finish(0)
        back(0).start()

    def events(*which):
        def run():
            for side, slot in which:
                event(side, slot)
        return run

    def come(side, slot):
        return lambda: arrive(side, slot)

    def nothing():
        return None

    w = wave
    order = [
        (0, w[0], events((0, w[1]), (1, w[1]))),
        (0, w[1], events((0, w[2]), (1, w[2]))),
        (0, w[2], events((0, w[3]), (1, w[3]))),
        (0, w[3], nothing),
        (1, w[0], nothing), (1, w[1], nothing), (1, w[2], nothing), (1, w[3], nothing),
        (0, 5, come(0, 5)), (0, 7, come(0, 7)), (1, 5, come(1, 5)), (1, 8, come(1, 8)), (0, 8, come(0, 8)),
        (0, 6, come(0, 6)), (1, 7, lambda: (low_done(), arrive(1, 7))), (1, 6, come(1, 6)),
    ]

    def visit(i, carry):
        side = jnp.int32(0)
        slot = jnp.int32(0)
        for n, (s, d, prepare) in enumerate(order):
            side = jnp.where(i == n, s, side)
            slot = jnp.where(i == n, d, slot)
            if prepare is not nothing:
                @pl.when(i == n)
                def _():
                    prepare()

        @pl.when(slot < plan.span)
        def _():
            sweep(side, slot)

        @pl.when(slot == plan.span)
        def _():
            sweep(side, slot, True, True)
        return carry

    lax.fori_loop(0, len(order), visit, 0)
    finish(1)
    back(1).start()

    first_col = pl.multiple_of(core * half_cols, half_cols)
    other_col = pl.multiple_of(other * half_cols, half_cols)
    out_ref[:, :, pl.ds(first_col, half_cols)] = ostage[0]
    for s in range(2):
        back(s).wait_recv()
        out_ref[s, :, pl.ds(other_col, half_cols)] = orecv[s]
    for s in range(2):
        back(s).wait_send()
    for copy in pair_kv + pair_q:
        copy.wait_send()
    for spec in sent:
        copy, ok = describe(*spec)

        @pl.when(ok)
        def _():
            copy.wait_send()


def attend(plan, hidden, w_q, cos, sin, kv_all):
    model_dim, heads, head_dim = w_q.shape
    _, _, _, heads_j, chunk, _ = kv_all.shape
    group = heads // (2 * heads_j)
    bf16, f32 = jnp.bfloat16, jnp.float32
    slots = plan.span + 1
    half_heads = heads // 2
    depth = model_dim // 4
    vmem = pl.BlockSpec(memory_space=pltpu.VMEM)
    anywhere = pl.BlockSpec(memory_space=pl.ANY)
    return pl.pallas_call(
        functools.partial(attention_kernel, plan),
        out_shape=jax.ShapeDtypeStruct((2, chunk, heads * head_dim), bf16),
        in_specs=[anywhere, anywhere, vmem, vmem, vmem],
        out_specs=vmem,
        scratch_shapes=[
            pltpu.VMEM((2, 2, heads_j, group, chunk, head_dim), bf16),
            pltpu.VMEM((2, heads_j, group, chunk, head_dim), bf16),
            pltpu.VMEM((2, slots, 2, 2, heads_j, chunk, head_dim), bf16),
            pltpu.VMEM((2, 2, heads_j, group, chunk, head_dim), f32),
            pltpu.VMEM((2, 2, heads_j, group, chunk, head_dim), f32),
            pltpu.VMEM((2, 2, heads_j, group, chunk, head_dim), f32),
            pltpu.VMEM((2, 2, chunk, heads_j * group * head_dim), bf16),
            pltpu.VMEM((2, chunk, heads_j * group * head_dim), bf16),
            pltpu.VMEM((2 * chunk, model_dim), bf16),
            pltpu.VMEM((MIX, MIX), bf16),
            pltpu.VMEM((2, depth, half_heads, head_dim), bf16),
            pltpu.VMEM((depth, half_heads * head_dim), bf16),
            pltpu.VMEM((2 * chunk, half_heads * head_dim), f32),
            pltpu.SemaphoreType.DMA((2,)),
            pltpu.SemaphoreType.DMA,
            pltpu.SemaphoreType.DMA((2,)),
            pltpu.SemaphoreType.DMA((6,)),
            pltpu.SemaphoreType.DMA((6,)),
            pltpu.SemaphoreType.DMA((64,)),
            pltpu.SemaphoreType.DMA((2, slots)),
        ],
        compiler_params=pltpu.CompilerParams(collective_id=0, has_side_effects=True, vmem_limit_bytes=62 * 1024 * 1024),
        name='attend',
    )(hidden, w_q.reshape(model_dim, 2, half_heads, head_dim), cos, sin, kv_all)


def solution(mesh):
    cp_size = mesh.shape['cp']
    plan = Plan(cp_size)

    def device_step(hidden, w_q, w_k, w_v, w_o):
        my_index = lax.axis_index('cp')
        chunk_len = hidden.shape[0] // 2
        model_dim = hidden.shape[1]
        heads, head_dim = w_q.shape[1], w_q.shape[2]
        chunk_ids = jnp.stack([my_index, 2 * cp_size - 1 - my_index])
        positions = (chunk_ids[:, None] * chunk_len + jnp.arange(chunk_len)[None, :]).reshape(2 * chunk_len)
        cos, sin = rotary_tables(positions, head_dim)
        kv_all = project_kv(hidden, w_k, w_v, cos, sin)
        attended = attend(plan, hidden, w_q, cos, sin, kv_all)
        out_rows = jnp.dot(attended.reshape(2 * chunk_len, heads * head_dim), w_o.reshape(heads * head_dim, model_dim), preferred_element_type=jnp.float32)
        return out_rows.astype(jnp.bfloat16)

    return jax.shard_map(device_step, mesh=mesh, in_specs=(P(('dp', 'cp'), None), P(), P(), P(), P()), out_specs=P(('dp', 'cp'), None), check_vma=False)
```

```python
import functools
import math

import jax
import jax.numpy as jnp
from jax import lax
from jax.experimental import pallas as pl
from jax.experimental.pallas import tpu as pltpu
from jax.sharding import PartitionSpec as P

WINDOW = 4096
ROPE_BASE = 10000.0
NEG = -jnp.inf


def rotary_tables(positions, head_dim):
    half_dim = head_dim // 2
    inv_freq = 1.0 / (ROPE_BASE ** (jnp.arange(half_dim, dtype=jnp.float32) * (2.0 / head_dim)))
    angles = positions.astype(jnp.float32)[:, None] * inv_freq
    cos_part = jnp.cos(angles)
    sin_part = jnp.sin(angles)
    return jnp.concatenate([cos_part, cos_part], axis=-1), jnp.concatenate([-sin_part, sin_part], axis=-1)


def spread(n_heads, size):
    per = size // n_heads
    to = lax.broadcasted_iota(jnp.int32, (size, size), 0)
    of = lax.broadcasted_iota(jnp.int32, (size, size), 1)
    return jnp.where((to % per) * n_heads + to // per == of, 1.0, 0.0).astype(jnp.bfloat16)


def by_head(mix, rows_ref, start, dst_ref, n_heads, base=0):
    size = mix.shape[0]
    per = size // n_heads
    if len(rows_ref.shape) == 3:
        first = pl.multiple_of(start // n_heads, 2 * per)
        pair = rows_ref[pl.ds(first, 2 * per)].reshape(2 * size, rows_ref.shape[2])
        wide = jnp.concatenate([pair[:size], pair[size:]], axis=1)
    else:
        wide = jnp.concatenate([rows_ref[pl.ds(start, size)], rows_ref[pl.ds(pl.multiple_of(start + size, size), size)]], axis=1)
    head_dim = wide.shape[1] // 2
    out = jnp.dot(mix, wide, preferred_element_type=jnp.float32).astype(jnp.bfloat16)
    at = base + pl.multiple_of(start // n_heads, 2 * per)
    for b in range(2):
        for h in range(n_heads):
            dst_ref[pl.ds(pl.multiple_of(at + b * per, per), per), h * head_dim:(h + 1) * head_dim] = out[h * per:(h + 1) * per, b * head_dim:(b + 1) * head_dim]


MIX = 256


def kv_kernel(n_heads, x_ref, wk_ref, wv_ref, cos_ref, sin_ref, out_ref, mix, wk, wv, acc_k, acc_v):
    step = pl.program_id(0)

    @pl.when(step == 0)
    def _():
        mix[...] = spread(n_heads, MIX)
        acc_k[...] = jnp.zeros_like(acc_k)
        acc_v[...] = jnp.zeros_like(acc_v)

    def arrange(i, carry):
        start = pl.multiple_of(i * (2 * MIX), 2 * MIX)
        by_head(mix[...], wk_ref, start, wk, n_heads)
        by_head(mix[...], wv_ref, start, wv, n_heads)
        return carry

    lax.fori_loop(0, wk_ref.shape[0] // (2 * MIX), arrange, 0, unroll=4)
    acc_k[...] += jnp.dot(x_ref[...], wk[...], preferred_element_type=jnp.float32)
    acc_v[...] += jnp.dot(x_ref[...], wv[...], preferred_element_type=jnp.float32)

    @pl.when(step == pl.num_programs(0) - 1)
    def _():
        chunk, head_dim = out_ref.shape[4], out_ref.shape[5]
        half = n_heads // 2
        for n in range(2):
            rows = slice(n * chunk, (n + 1) * chunk)
            for h in range(n_heads):
                cols = slice(h * head_dim, (h + 1) * head_dim)
                k = acc_k[rows, cols].astype(jnp.bfloat16).astype(jnp.float32)
                k = k * cos_ref[rows] + pltpu.roll(k, head_dim // 2, 1) * sin_ref[rows]
                out_ref[h // half, n, 0, h % half] = k.astype(jnp.bfloat16)
                out_ref[h // half, n, 1, h % half] = acc_v[rows, cols].astype(jnp.bfloat16)


def project_kv(hidden, w_k, w_v, cos, sin):
    rows, model_dim = hidden.shape
    n_heads, head_dim = w_k.shape[1:]
    chunk = rows // 2
    depth = model_dim // 4
    bf16, f32 = jnp.bfloat16, jnp.float32
    cols = n_heads * head_dim
    return pl.pallas_call(
        functools.partial(kv_kernel, n_heads),
        grid=(model_dim // depth,),
        in_specs=[
            pl.BlockSpec((rows, depth), lambda i: (0, i)),
            pl.BlockSpec((depth * n_heads, head_dim), lambda i: (i, 0)),
            pl.BlockSpec((depth * n_heads, head_dim), lambda i: (i, 0)),
            pl.BlockSpec((rows, head_dim), lambda i: (0, 0)),
            pl.BlockSpec((rows, head_dim), lambda i: (0, 0)),
        ],
        out_specs=pl.BlockSpec((2, 2, 2, n_heads // 2, chunk, head_dim), lambda i: (0, 0, 0, 0, 0, 0)),
        out_shape=jax.ShapeDtypeStruct((2, 2, 2, n_heads // 2, chunk, head_dim), bf16),
        scratch_shapes=[
            pltpu.VMEM((MIX, MIX), bf16),
            pltpu.VMEM((depth, cols), bf16),
            pltpu.VMEM((depth, cols), bf16),
            pltpu.VMEM((rows, cols), f32),
            pltpu.VMEM((rows, cols), f32),
        ],
        compiler_params=pltpu.CompilerParams(dimension_semantics=('arbitrary',), vmem_limit_bytes=62 * 1024 * 1024),
        name='project_kv',
    )(hidden, w_k.reshape(model_dim * n_heads, head_dim), w_v.reshape(model_dim * n_heads, head_dim), cos, sin)


class Plan:
    def __init__(self, cp_size):
        self.chips = cp_size // 2
        self.row = math.isqrt(self.chips)
        self.span = 2 * self.row

    def pair(self, chip, side):
        return jnp.where(side == 0, chip, 2 * self.chips - 1 - chip)

    def chip_of(self, pair):
        return jnp.where(pair < self.chips, pair, 2 * self.chips - 1 - pair)

    def side_of(self, pair):
        return jnp.where(pair < self.chips, 0, 1)

    def twin(self, pair, slot):
        same = 2 * self.chip_of(pair) + slot - (2 * self.chips - 1)
        return jnp.where(pair < self.chips, -1, same)


def attention_kernel(plan, x_hbm, wq_ref, cos_in, sin_in, kv_ref, out_ref, qbuf, kvbuf, acc, m_ref, l_ref,
                     ostage, orecv, x_ref, turns, mix, wraw, wsort, loc_sem, x_sem, w_sem, pair_send, pair_recv, send_sem, recv_sem):
    me = lax.axis_index('cp')
    chip = me // 2
    core = lax.rem(me, 2)
    other = 1 - core
    row = plan.row
    x = lax.rem(chip, row)
    y = chip // row
    n_row = plan.chips // row
    chunk = qbuf.shape[4]
    heads_j = qbuf.shape[2]
    group = qbuf.shape[3]
    head_dim = qbuf.shape[5]
    half_cols = heads_j * group * head_dim

    def device(target_chip, target_core):
        return {'cp': target_chip * 2 + target_core}

    barrier = pltpu.get_barrier_semaphore()
    pl.semaphore_signal(barrier, inc=1, device_id=device(chip, other), device_id_type=pl.DeviceIdType.MESH)
    for step in range(1, row):
        mate = y * row + lax.rem(x + step, row)
        pl.semaphore_signal(barrier, inc=1, device_id=device(mate, core), device_id_type=pl.DeviceIdType.MESH)
    for dy in (-1, 1):
        @pl.when((y + dy >= 0) & (y + dy < n_row))
        def _():
            pl.semaphore_signal(barrier, inc=1, device_id=device(chip + dy * row, core), device_id_type=pl.DeviceIdType.MESH)
    pl.semaphore_wait(barrier, row + jnp.where(y > 0, 1, 0) + jnp.where(y < n_row - 1, 1, 0))

    partner = device(chip, other)
    pairs = [plan.pair(chip, s) for s in range(2)]
    own_sub = [core, other]

    n_heads = heads_j * group
    depth = wraw.shape[1]
    n_blocks = wq_ref.shape[0] // depth
    load_x = pltpu.make_async_copy(x_hbm, x_ref.at[0], x_sem)

    def fetch(block):
        at = pl.multiple_of(block * depth, depth)
        slot = lax.rem(block, 2)
        return pltpu.make_async_copy(wq_ref.at[pl.ds(at, depth), core], wraw.at[slot], w_sem.at[slot])

    fetch(0).start()

    pair_kv = []
    local = []
    for s in range(2):
        pair_kv.append(pltpu.make_async_remote_copy(
            src_ref=kv_ref.at[other, s], dst_ref=kvbuf.at[s, 0, own_sub[s]], send_sem=pair_send.at[s],
            recv_sem=pair_recv.at[s], device_id=partner, device_id_type=pl.DeviceIdType.MESH))
        local.append(pltpu.make_async_copy(kv_ref.at[core, s], kvbuf.at[s, 0, own_sub[s]], loc_sem.at[s]))
    for copy in pair_kv + local:
        copy.start()
    pair_x = pltpu.make_async_remote_copy(
        src_ref=x_hbm, dst_ref=x_ref.at[1], send_sem=pair_send.at[2], recv_sem=pair_recv.at[2],
        device_id=partner, device_id_type=pl.DeviceIdType.MESH)
    pair_x.start()
    load_x.start()
    pair_turn = []
    for t, table in enumerate((cos_in, sin_in)):
        local.append(pltpu.make_async_copy(table, turns.at[0, t], loc_sem.at[2 + t]))
        local[-1].start()
        pair_turn.append(pltpu.make_async_remote_copy(
            src_ref=table, dst_ref=turns.at[1, t], send_sem=pair_send.at[6 + t], recv_sem=pair_recv.at[6 + t],
            device_id=partner, device_id_type=pl.DeviceIdType.MESH))
        pair_turn[-1].start()

    acc[...] = jnp.zeros_like(acc)
    l_ref[...] = jnp.zeros_like(l_ref)
    m_ref[...] = jnp.full_like(m_ref, NEG)

    def held(side, slot):
        twin = plan.twin(pairs[side], slot)
        return (jnp.where(twin >= 0, 0, side), jnp.where(twin >= 0, twin, slot))

    sent = []

    def along(side, step):
        col = lax.rem(pairs[side], row)
        return lax.rem(col + step, row) - col

    def describe(index, side, slot, where, cond):
        delta = where()
        node = pairs[side] + delta
        goal = slot + delta
        ok = (node < 2 * plan.chips) & (pairs[side] - slot >= 0) & (plan.twin(node, goal) < 0) & cond()
        held_side, held_slot = held(side, slot)
        copy = pltpu.make_async_remote_copy(
            src_ref=kvbuf.at[held_side, held_slot], dst_ref=kvbuf.at[plan.side_of(node), goal],
            send_sem=send_sem.at[index], recv_sem=recv_sem.at[plan.side_of(node), goal],
            device_id=device(plan.chip_of(node), core), device_id_type=pl.DeviceIdType.MESH)
        return copy, ok

    def send(side, slot, where, cond):
        spec = (len(sent), side, slot, where, cond)
        sent.append(spec)
        copy, ok = describe(*spec)

        @pl.when(ok)
        def _():
            copy.start()

    def arrive(side, slot, extra=True):
        ok = (pairs[side] - slot >= 0) & (plan.twin(pairs[side], slot) < 0) & extra

        @pl.when(ok)
        def _():
            buf = kvbuf.at[side, slot]
            pltpu.make_async_remote_copy(
                src_ref=buf, dst_ref=buf, send_sem=send_sem.at[0], recv_sem=recv_sem.at[side, slot],
                device_id=partner, device_id_type=pl.DeviceIdType.MESH).wait_recv()

    def always():
        return pairs[0] >= 0

    def down():
        return row

    for copy in pair_kv:
        copy.wait_recv()
    for copy in local:
        copy.wait()
    near, far = 1, row - 1

    def col_of(side):
        return lax.rem(pairs[side], row)

    def inner(side):
        return (col_of(side) > 0) & (col_of(side) < row - 1)

    def launch(side, slot, cond):
        send(side, slot, down, cond)
        if slot == 0 or slot == row:
            for step in (1, row - 1):
                where = functools.partial(along, side, step)
                send(side, slot, where, lambda w=where: cond() & ((w() > 0) if slot == 0 else (w() < 0)))
        elif slot == near:
            send(side, slot, lambda: 1, lambda: cond() & inner(side))
        elif slot == far:
            send(side, slot, lambda: -1, lambda: cond() & inner(side))

    def echo(slot, cond=lambda: pairs[0] >= 0):
        def as_high(d):
            return plan.twin(pairs[1], d) == slot
        for d in range(1, row + 1):
            if (d - slot) % 2 == 1 and d > slot:
                send(1, d, down, lambda d=d: as_high(d) & cond())

    def event(side, slot, cond=always):
        arrive(side, slot, cond())
        if side == 0:
            launch(0, slot, cond)
            echo(slot, cond)
        else:
            launch(1, slot, lambda: cond() & (plan.twin(pairs[1], slot) < 0))

    launch(0, 0, always)
    launch(1, 0, always)
    echo(0)

    mix[...] = spread(n_heads, MIX)

    def sort(block, carry):
        fetch(block).wait()

        @pl.when(block + 1 < n_blocks)
        def _():
            fetch(block + 1).start()

        raw = wraw.at[lax.rem(block, 2)]
        base = pl.multiple_of(block * depth, depth)

        def arrange(i, c):
            by_head(mix[...], raw, pl.multiple_of(i * (2 * MIX), 2 * MIX), wsort, n_heads, base)
            return c

        lax.fori_loop(0, depth * n_heads // (2 * MIX), arrange, 0, unroll=8)
        return carry

    lax.fori_loop(0, n_blocks, sort, 0)
    load_x.wait()
    wide = 2
    per_rows = n_heads // wide

    def project(i, carry):
        whose = i // per_rows
        first = lax.rem(i, per_rows) * wide

        @pl.when(i == per_rows)
        def _():
            pair_x.wait_recv()
            for copy in pair_turn:
                copy.wait_recv()

        cols = pl.ds(pl.multiple_of(first * head_dim, wide * head_dim), wide * head_dim)
        part = jnp.dot(x_ref[whose], wsort[:, cols], preferred_element_type=jnp.float32)
        for s in range(2):
            rows = slice(s * chunk, (s + 1) * chunk)
            sub = jnp.where(whose == 0, own_sub[s], 1 - own_sub[s])
            for h in range(wide):
                q = part[rows, h * head_dim:(h + 1) * head_dim].astype(jnp.bfloat16).astype(jnp.float32)
                q = q * turns[whose, 0, rows] + pltpu.roll(q, head_dim // 2, 1) * turns[whose, 1, rows]
                qbuf[s, sub, first // group, lax.rem(first, group) + h] = (q * head_dim ** -0.5).astype(jnp.bfloat16)

        @pl.when(i == 2 * per_rows - 2)
        def _():
            event(0, row)
            event(1, row)
        return carry

    lax.fori_loop(0, 2 * per_rows, project, 0)

    def block(side, slot_side, slot, j, subs, masked, edge):
        k = kvbuf[slot_side, slot, :, 0, j].reshape(2 * chunk, head_dim)
        v = kvbuf[slot_side, slot, :, 1, j].reshape(2 * chunk, head_dim)
        tiles = [(a, g) for a in subs for g in range(group)]

        def score(t):
            a, g = tiles[t]
            return lax.dot_general(qbuf[side, a, j, g], k, (((1,), (1,)), ((), ())), preferred_element_type=jnp.float32)

        def update(t, s):
            a, g = tiles[t]
            if masked:
                rows = lax.broadcasted_iota(jnp.int32, (chunk, 2 * chunk), 0) + a * chunk
                cols = lax.broadcasted_iota(jnp.int32, (chunk, 2 * chunk), 1)
                s = jnp.where((cols > rows) if edge else (cols <= rows), s, NEG)
            m_old = m_ref[side, a, j, g]
            m_new = jnp.maximum(m_old, jnp.max(s, axis=1, keepdims=True))
            alpha = jnp.exp(m_old - m_new)
            e = jnp.exp(s - jnp.concatenate([m_new] * (2 * chunk // m_new.shape[1]), axis=1))
            part = e[:, :head_dim]
            for b in range(1, 2 * chunk // head_dim):
                part = part + e[:, b * head_dim:(b + 1) * head_dim]
            m_ref[side, a, j, g] = m_new
            l_ref[side, a, j, g] = l_ref[side, a, j, g] * alpha + part
            acc[side, a, j, g] = acc[side, a, j, g] * alpha + jnp.dot(e.astype(jnp.bfloat16), v, preferred_element_type=jnp.float32)

        ahead = 2
        scores = [score(t) for t in range(ahead)]
        for t in range(len(tiles)):
            if t + ahead < len(tiles):
                scores.append(score(t + ahead))
            update(t, scores[t])

    def sweep(side, slot, masked=False, edge=False):
        slot_side, at = held(side, slot) if isinstance(side, int) else (
            jnp.where(plan.twin(jnp.where(side == 0, pairs[0], pairs[1]), slot) >= 0, 0, side),
            jnp.where(plan.twin(jnp.where(side == 0, pairs[0], pairs[1]), slot) >= 0,
                      plan.twin(jnp.where(side == 0, pairs[0], pairs[1]), slot), slot))
        mine = jnp.where(side == 0, pairs[0], pairs[1])

        @pl.when(mine - slot >= 0)
        def _():
            def body(i, carry):
                block(side, slot_side, at, i, (0, 1), masked, edge)
                return carry
            lax.fori_loop(0, heads_j, body, 0)

    for s in range(2):
        event(s, near, lambda s=s: col_of(s) > 0)
    lax.fori_loop(0, 2, lambda s, c: (sweep(s, 0, True, False), c)[1], 0)

    def finish(s):
        def body(i, carry):
            a = jnp.where(i == 0, 1 - own_sub[s], own_sub[s])
            for j in range(heads_j):
                for g in range(group):
                    total = jnp.sum(l_ref[s, a, j, g], axis=1, keepdims=True)
                    o = (acc[s, a, j, g] / total).astype(jnp.bfloat16)
                    col = (j * group + g) * head_dim
                    ostage[1 - i, s, :, col:col + head_dim] = o
            return carry

        lax.fori_loop(0, 2, body, 0)

    def back(s):
        return pltpu.make_async_remote_copy(
            src_ref=ostage.at[1, s], dst_ref=orecv.at[s], send_sem=pair_send.at[4 + s], recv_sem=pair_recv.at[4 + s],
            device_id=partner, device_id_type=pl.DeviceIdType.MESH)

    def low_done():
        finish(0)
        back(0).start()

    def come(*which):
        def run():
            for side, slot in which:
                arrive(side, slot)
        return run

    def far_events():
        for s in range(2):
            event(s, far)
        for s in range(2):
            event(s, near, lambda s=s: col_of(s) == 0)

    def nothing():
        return None

    order = [
        (0, row, 0, nothing), (1, row, 1, nothing),
        (0, near, 0, far_events), (1, near, 0, nothing), (0, far, 0, nothing), (1, far, 1, nothing),
        (1, 2, 0, lambda: event(1, 2)), (0, 8, 0, come((0, 8))), (0, 2, 0, lambda: event(0, 2)),
        (1, row, 2, nothing), (1, far, 2, nothing),
        (0, 5, 0, come((0, 5))), (1, 5, 0, come((1, 5))), (0, 7, 0, come((0, 7))), (1, 8, 0, come((1, 8))),
        (0, 6, 0, come((0, 6))), (1, 7, 0, lambda: (low_done(), arrive(1, 7))), (1, 6, 0, come((1, 6))),
    ]

    def visit(i, carry):
        side = jnp.int32(0)
        slot = jnp.int32(0)
        kind = jnp.int32(0)
        for n, (s, d, when, prepare) in enumerate(order):
            side = jnp.where(i == n, s, side)
            slot = jnp.where(i == n, d, slot)
            kind = jnp.where(i == n, when, kind)
            if prepare is not nothing:
                @pl.when(i == n)
                def _():
                    prepare()

        doubled = plan.twin(jnp.where(side == 0, pairs[0], pairs[1]), slot) >= 0
        due = (kind == 0) | ((kind == 1) & jnp.logical_not(doubled)) | ((kind == 2) & doubled)

        @pl.when(due & (slot < plan.span))
        def _():
            sweep(side, slot)

        @pl.when(due & (slot == plan.span))
        def _():
            sweep(side, slot, True, True)
        return carry

    lax.fori_loop(0, len(order), visit, 0)
    finish(1)
    back(1).start()

    first_col = pl.multiple_of(core * half_cols, half_cols)
    other_col = pl.multiple_of(other * half_cols, half_cols)
    out_ref[:, :, pl.ds(first_col, half_cols)] = ostage[0]
    for s in range(2):
        back(s).wait_recv()
        out_ref[s, :, pl.ds(other_col, half_cols)] = orecv[s]
    for s in range(2):
        back(s).wait_send()
    for copy in pair_kv + [pair_x] + pair_turn:
        copy.wait_send()
    for spec in sent:
        copy, ok = describe(*spec)

        @pl.when(ok)
        def _():
            copy.wait_send()


def attend(plan, hidden, w_q, cos, sin, kv_all):
    model_dim, heads, head_dim = w_q.shape
    _, _, _, heads_j, chunk, _ = kv_all.shape
    group = heads // (2 * heads_j)
    bf16, f32 = jnp.bfloat16, jnp.float32
    slots = plan.span + 1
    half_heads = heads // 2
    depth = model_dim // 4
    vmem = pl.BlockSpec(memory_space=pltpu.VMEM)
    anywhere = pl.BlockSpec(memory_space=pl.ANY)
    return pl.pallas_call(
        functools.partial(attention_kernel, plan),
        out_shape=jax.ShapeDtypeStruct((2, chunk, heads * head_dim), bf16),
        in_specs=[anywhere, anywhere, vmem, vmem, vmem],
        out_specs=vmem,
        scratch_shapes=[
            pltpu.VMEM((2, 2, heads_j, group, chunk, head_dim), bf16),
            pltpu.VMEM((2, slots, 2, 2, heads_j, chunk, head_dim), bf16),
            pltpu.VMEM((2, 2, heads_j, group, chunk, head_dim), f32),
            pltpu.VMEM((2, 2, heads_j, group, chunk, head_dim), f32),
            pltpu.VMEM((2, 2, heads_j, group, chunk, head_dim), f32),
            pltpu.VMEM((2, 2, chunk, heads_j * group * head_dim), bf16),
            pltpu.VMEM((2, chunk, heads_j * group * head_dim), bf16),
            pltpu.VMEM((2, 2 * chunk, model_dim), bf16),
            pltpu.VMEM((2, 2, 2 * chunk, head_dim), f32),
            pltpu.VMEM((MIX, MIX), bf16),
            pltpu.VMEM((2, depth, half_heads, head_dim), bf16),
            pltpu.VMEM((model_dim, half_heads * head_dim), bf16),
            pltpu.SemaphoreType.DMA((4,)),
            pltpu.SemaphoreType.DMA,
            pltpu.SemaphoreType.DMA((2,)),
            pltpu.SemaphoreType.DMA((8,)),
            pltpu.SemaphoreType.DMA((8,)),
            pltpu.SemaphoreType.DMA((64,)),
            pltpu.SemaphoreType.DMA((2, slots)),
        ],
        compiler_params=pltpu.CompilerParams(collective_id=0, has_side_effects=True, vmem_limit_bytes=62 * 1024 * 1024),
        name='attend',
    )(hidden, w_q.reshape(model_dim, 2, half_heads, head_dim), cos, sin, kv_all)


def solution(mesh):
    cp_size = mesh.shape['cp']
    plan = Plan(cp_size)

    def device_step(hidden, w_q, w_k, w_v, w_o):
        my_index = lax.axis_index('cp')
        chunk_len = hidden.shape[0] // 2
        model_dim = hidden.shape[1]
        heads, head_dim = w_q.shape[1], w_q.shape[2]
        chunk_ids = jnp.stack([my_index, 2 * cp_size - 1 - my_index])
        positions = (chunk_ids[:, None] * chunk_len + jnp.arange(chunk_len)[None, :]).reshape(2 * chunk_len)
        cos, sin = rotary_tables(positions, head_dim)
        kv_all = project_kv(hidden, w_k, w_v, cos, sin)
        attended = attend(plan, hidden, w_q, cos, sin, kv_all)
        out_rows = jnp.dot(attended.reshape(2 * chunk_len, heads * head_dim), w_o.reshape(heads * head_dim, model_dim), preferred_element_type=jnp.float32)
        return out_rows.astype(jnp.bfloat16)

    return jax.shard_map(device_step, mesh=mesh, in_specs=(P(('dp', 'cp'), None), P(), P(), P(), P()), out_specs=P(('dp', 'cp'), None), check_vma=False)
```

```python
import functools
import math

import jax
import jax.numpy as jnp
from jax import lax
from jax.experimental import pallas as pl
from jax.experimental.pallas import tpu as pltpu
from jax.sharding import PartitionSpec as P

WINDOW = 4096
ROPE_BASE = 10000.0
NEG = -jnp.inf


def rotary_tables(positions, head_dim):
    half_dim = head_dim // 2
    inv_freq = 1.0 / (ROPE_BASE ** (jnp.arange(half_dim, dtype=jnp.float32) * (2.0 / head_dim)))
    angles = positions.astype(jnp.float32)[:, None] * inv_freq
    cos_part = jnp.cos(angles)
    sin_part = jnp.sin(angles)
    return jnp.concatenate([cos_part, cos_part], axis=-1), jnp.concatenate([-sin_part, sin_part], axis=-1)


def spread(n_heads, size):
    per = size // n_heads
    to = lax.broadcasted_iota(jnp.int32, (size, size), 0)
    of = lax.broadcasted_iota(jnp.int32, (size, size), 1)
    return jnp.where((to % per) * n_heads + to // per == of, 1.0, 0.0).astype(jnp.bfloat16)


def by_head(mix, rows_ref, start, dst_ref, n_heads, base, col):
    size = mix.shape[0]
    per = size // n_heads
    head_dim = rows_ref.shape[2]
    first = pl.multiple_of(start // rows_ref.shape[1], 2 * size // rows_ref.shape[1])
    pair = rows_ref[pl.ds(first, 2 * size // rows_ref.shape[1])].reshape(2 * size, head_dim)
    wide = jnp.concatenate([pair[:size], pair[size:]], axis=1)
    out = jnp.dot(mix, wide, preferred_element_type=jnp.float32).astype(jnp.bfloat16)
    at = base + pl.multiple_of(start // n_heads, 2 * per)
    for b in range(2):
        for h in range(n_heads):
            cols = pl.ds(pl.multiple_of(col + h * head_dim, head_dim), head_dim)
            dst_ref[pl.ds(pl.multiple_of(at + b * per, per), per), cols] = out[h * per:(h + 1) * per, b * head_dim:(b + 1) * head_dim]


MIX = 256


class Plan:
    def __init__(self, cp_size):
        self.chips = cp_size // 2
        self.row = math.isqrt(self.chips)
        self.span = 2 * self.row

    def pair(self, chip, side):
        return jnp.where(side == 0, chip, 2 * self.chips - 1 - chip)

    def chip_of(self, pair):
        return jnp.where(pair < self.chips, pair, 2 * self.chips - 1 - pair)

    def side_of(self, pair):
        return jnp.where(pair < self.chips, 0, 1)

    def twin(self, pair, slot):
        same = 2 * self.chip_of(pair) + slot - (2 * self.chips - 1)
        return jnp.where(pair < self.chips, -1, same)


def attention_kernel(plan, kv_heads, x_hbm, wk_ref, wv_ref, wq_ref, cos_in, sin_in, out_ref, kv_ref, qbuf, kvbuf, acc, m_ref, l_ref,
                     ostage, orecv, x_ref, turns, mix, wraw, wsort, loc_sem, x_sem, w_sem, pair_send, pair_recv, send_sem, recv_sem):
    me = lax.axis_index('cp')
    chip = me // 2
    core = lax.rem(me, 2)
    other = 1 - core
    row = plan.row
    x = lax.rem(chip, row)
    y = chip // row
    n_row = plan.chips // row
    chunk = qbuf.shape[4]
    heads_j = qbuf.shape[2]
    group = qbuf.shape[3]
    head_dim = qbuf.shape[5]
    half_cols = heads_j * group * head_dim

    def device(target_chip, target_core):
        return {'cp': target_chip * 2 + target_core}

    barrier = pltpu.get_barrier_semaphore()
    pl.semaphore_signal(barrier, inc=1, device_id=device(chip, other), device_id_type=pl.DeviceIdType.MESH)
    for step in range(1, row):
        mate = y * row + lax.rem(x + step, row)
        pl.semaphore_signal(barrier, inc=1, device_id=device(mate, core), device_id_type=pl.DeviceIdType.MESH)
    for dy in (-1, 1):
        @pl.when((y + dy >= 0) & (y + dy < n_row))
        def _():
            pl.semaphore_signal(barrier, inc=1, device_id=device(chip + dy * row, core), device_id_type=pl.DeviceIdType.MESH)

    partner = device(chip, other)
    pairs = [plan.pair(chip, s) for s in range(2)]
    own_sub = [core, other]

    n_heads = heads_j * group
    depth = wraw.shape[1]
    n_kv = wk_ref.shape[0] // depth
    n_q = wq_ref.shape[0] // depth
    load_x = pltpu.make_async_copy(x_hbm, x_ref.at[0], x_sem)

    def fetch(block, part):
        at = pl.ds(pl.multiple_of(block * depth, depth), depth)
        slot = lax.rem(block, 2)
        src = (wk_ref.at[at], wv_ref.at[at], wq_ref.at[at, core] if part == 2 else None)[part]
        return pltpu.make_async_copy(src, wraw.at[slot], w_sem.at[slot])

    fetch(0, 0).start()
    load_x.start()

    acc[...] = jnp.zeros_like(acc)
    l_ref[...] = jnp.zeros_like(l_ref)
    m_ref[...] = jnp.full_like(m_ref, NEG)

    mix[...] = spread(kv_heads, MIX)
    width = kv_heads * head_dim

    def sort(part, blocks, heads, follow):
        def step(block, carry):
            fetch(block, part).wait()

            @pl.when(block + 1 < blocks)
            def _():
                fetch(block + 1, part).start()

            @pl.when(block + 1 == blocks)
            def _():
                follow()

            raw = wraw.at[lax.rem(block, 2)]
            rows = depth * raw.shape[1] // heads
            base = pl.multiple_of(block * rows, rows)

            def arrange(i, c):
                by_head(mix[...], raw, pl.multiple_of(i * (2 * MIX), 2 * MIX), wsort, heads, base, width if part == 1 else 0)
                return c

            lax.fori_loop(0, depth * raw.shape[1] // (2 * MIX), arrange, 0, unroll=8)
            return carry

        lax.fori_loop(0, blocks, step, 0)

    sort(0, n_kv, kv_heads, lambda: fetch(0, 1).start())
    pl.semaphore_wait(barrier, row + jnp.where(y > 0, 1, 0) + jnp.where(y < n_row - 1, 1, 0))
    pair_x = pltpu.make_async_remote_copy(
        src_ref=x_hbm, dst_ref=x_ref.at[1], send_sem=pair_send.at[2], recv_sem=pair_recv.at[2],
        device_id=partner, device_id_type=pl.DeviceIdType.MESH)
    pair_x.start()
    sort(1, n_kv, kv_heads, lambda: fetch(0, 2).start())
    load_x.wait()
    wide = 2

    def project_kv(i, carry):
        first = lax.rem(i, kv_heads // wide)
        is_key = i < kv_heads // wide
        cols = pl.ds(pl.multiple_of(i * wide * head_dim, wide * head_dim), wide * head_dim)
        part = jnp.dot(x_ref[0], wsort[:, cols], preferred_element_type=jnp.float32)
        for s in range(2):
            rows = slice(s * chunk, (s + 1) * chunk)
            for h in range(wide):
                plain = part[rows, h * head_dim:(h + 1) * head_dim].astype(jnp.bfloat16).astype(jnp.float32)
                turned = plain * cos_in[rows] + pltpu.roll(plain, head_dim // 2, 1) * sin_in[rows]
                kv_ref[first, s, jnp.where(is_key, 0, 1), h] = jnp.where(is_key, turned, plain).astype(jnp.bfloat16)
        return carry

    lax.fori_loop(0, 2 * kv_heads // wide, project_kv, 0)

    pair_kv = []
    local = []
    for s in range(2):
        pair_kv.append(pltpu.make_async_remote_copy(
            src_ref=kv_ref.at[other, s], dst_ref=kvbuf.at[s, 0, own_sub[s]], send_sem=pair_send.at[s],
            recv_sem=pair_recv.at[s], device_id=partner, device_id_type=pl.DeviceIdType.MESH))
        local.append(pltpu.make_async_copy(kv_ref.at[core, s], kvbuf.at[s, 0, own_sub[s]], loc_sem.at[s]))
    for copy in pair_kv + local:
        copy.start()
    pair_turn = []
    for t, table in enumerate((cos_in, sin_in)):
        local.append(pltpu.make_async_copy(table, turns.at[0, t], loc_sem.at[2 + t]))
        local[-1].start()
        pair_turn.append(pltpu.make_async_remote_copy(
            src_ref=table, dst_ref=turns.at[1, t], send_sem=pair_send.at[6 + t], recv_sem=pair_recv.at[6 + t],
            device_id=partner, device_id_type=pl.DeviceIdType.MESH))
        pair_turn[-1].start()

    def held(side, slot):
        twin = plan.twin(pairs[side], slot)
        return (jnp.where(twin >= 0, 0, side), jnp.where(twin >= 0, twin, slot))

    sent = []

    def along(side, step):
        col = lax.rem(pairs[side], row)
        return lax.rem(col + step, row) - col

    def describe(index, side, slot, where, cond):
        delta = where()
        node = pairs[side] + delta
        goal = slot + delta
        ok = (node < 2 * plan.chips) & (pairs[side] - slot >= 0) & (plan.twin(node, goal) < 0) & cond()
        held_side, held_slot = held(side, slot)
        copy = pltpu.make_async_remote_copy(
            src_ref=kvbuf.at[held_side, held_slot], dst_ref=kvbuf.at[plan.side_of(node), goal],
            send_sem=send_sem.at[index], recv_sem=recv_sem.at[plan.side_of(node), goal],
            device_id=device(plan.chip_of(node), core), device_id_type=pl.DeviceIdType.MESH)
        return copy, ok

    def send(side, slot, where, cond):
        spec = (len(sent), side, slot, where, cond)
        sent.append(spec)
        copy, ok = describe(*spec)

        @pl.when(ok)
        def _():
            copy.start()

    def arrive(side, slot, extra=True):
        ok = (pairs[side] - slot >= 0) & (plan.twin(pairs[side], slot) < 0) & extra

        @pl.when(ok)
        def _():
            buf = kvbuf.at[side, slot]
            pltpu.make_async_remote_copy(
                src_ref=buf, dst_ref=buf, send_sem=send_sem.at[0], recv_sem=recv_sem.at[side, slot],
                device_id=partner, device_id_type=pl.DeviceIdType.MESH).wait_recv()

    def always():
        return pairs[0] >= 0

    def down():
        return row

    for copy in pair_kv:
        copy.wait_recv()
    for copy in local:
        copy.wait()
    near, far = 1, row - 1

    def col_of(side):
        return lax.rem(pairs[side], row)

    def inner(side):
        return (col_of(side) > 0) & (col_of(side) < row - 1)

    def launch(side, slot, cond):
        send(side, slot, down, cond)
        if slot == 0 or slot == row:
            for step in (1, row - 1):
                where = functools.partial(along, side, step)
                send(side, slot, where, lambda w=where: cond() & ((w() > 0) if slot == 0 else (w() < 0)))
        elif slot == near:
            send(side, slot, lambda: 1, lambda: cond() & inner(side))
        elif slot == far:
            send(side, slot, lambda: -1, lambda: cond() & inner(side))

    def echo(slot, cond=lambda: pairs[0] >= 0):
        def as_high(d):
            return plan.twin(pairs[1], d) == slot
        for d in range(1, row + 1):
            if (d - slot) % 2 == 1 and d > slot:
                send(1, d, down, lambda d=d: as_high(d) & cond())

    def event(side, slot, cond=always):
        arrive(side, slot, cond())
        if side == 0:
            launch(0, slot, cond)
            echo(slot, cond)
        else:
            launch(1, slot, lambda: cond() & (plan.twin(pairs[1], slot) < 0))

    launch(0, 0, always)
    launch(1, 0, always)
    echo(0)

    mix[...] = spread(n_heads, MIX)
    sort(2, n_q, n_heads, lambda: None)
    per_rows = n_heads // wide

    def project(i, carry):
        whose = i // per_rows
        first = lax.rem(i, per_rows) * wide

        @pl.when(i == per_rows)
        def _():
            pair_x.wait_recv()
            for copy in pair_turn:
                copy.wait_recv()

        cols = pl.ds(pl.multiple_of(first * head_dim, wide * head_dim), wide * head_dim)
        part = jnp.dot(x_ref[whose], wsort[:, cols], preferred_element_type=jnp.float32)
        for s in range(2):
            rows = slice(s * chunk, (s + 1) * chunk)
            sub = jnp.where(whose == 0, own_sub[s], 1 - own_sub[s])
            for h in range(wide):
                q = part[rows, h * head_dim:(h + 1) * head_dim].astype(jnp.bfloat16).astype(jnp.float32)
                q = q * turns[whose, 0, rows] + pltpu.roll(q, head_dim // 2, 1) * turns[whose, 1, rows]
                qbuf[s, sub, first // group, lax.rem(first, group) + h] = (q * head_dim ** -0.5).astype(jnp.bfloat16)

        @pl.when(i == 2 * per_rows - 2)
        def _():
            event(0, row)
            event(1, row)
        return carry

    lax.fori_loop(0, 2 * per_rows, project, 0)

    def block(side, slot_side, slot, j, subs, masked, edge):
        k = kvbuf[slot_side, slot, :, 0, j].reshape(2 * chunk, head_dim)
        v = kvbuf[slot_side, slot, :, 1, j].reshape(2 * chunk, head_dim)
        tiles = [(a, g) for a in subs for g in range(group)]

        def score(t):
            a, g = tiles[t]
            return lax.dot_general(qbuf[side, a, j, g], k, (((1,), (1,)), ((), ())), preferred_element_type=jnp.float32)

        def update(t, s):
            a, g = tiles[t]
            if masked:
                rows = lax.broadcasted_iota(jnp.int32, (chunk, 2 * chunk), 0) + a * chunk
                cols = lax.broadcasted_iota(jnp.int32, (chunk, 2 * chunk), 1)
                s = jnp.where((cols > rows) if edge else (cols <= rows), s, NEG)
            m_old = m_ref[side, a, j, g]
            m_new = jnp.maximum(m_old, jnp.max(s, axis=1, keepdims=True))
            alpha = jnp.exp(m_old - m_new)
            e = jnp.exp(s - jnp.concatenate([m_new] * (2 * chunk // m_new.shape[1]), axis=1))
            part = e[:, :head_dim]
            for b in range(1, 2 * chunk // head_dim):
                part = part + e[:, b * head_dim:(b + 1) * head_dim]
            m_ref[side, a, j, g] = m_new
            l_ref[side, a, j, g] = l_ref[side, a, j, g] * alpha + part
            acc[side, a, j, g] = acc[side, a, j, g] * alpha + jnp.dot(e.astype(jnp.bfloat16), v, preferred_element_type=jnp.float32)

        ahead = 2
        scores = [score(t) for t in range(ahead)]
        for t in range(len(tiles)):
            if t + ahead < len(tiles):
                scores.append(score(t + ahead))
            update(t, scores[t])

    def sweep(side, slot, masked=False, edge=False):
        slot_side, at = held(side, slot) if isinstance(side, int) else (
            jnp.where(plan.twin(jnp.where(side == 0, pairs[0], pairs[1]), slot) >= 0, 0, side),
            jnp.where(plan.twin(jnp.where(side == 0, pairs[0], pairs[1]), slot) >= 0,
                      plan.twin(jnp.where(side == 0, pairs[0], pairs[1]), slot), slot))
        mine = jnp.where(side == 0, pairs[0], pairs[1])

        @pl.when(mine - slot >= 0)
        def _():
            def body(i, carry):
                block(side, slot_side, at, i, (0, 1), masked, edge)
                return carry
            lax.fori_loop(0, heads_j, body, 0)

    for s in range(2):
        event(s, near, lambda s=s: col_of(s) > 0)
    lax.fori_loop(0, 2, lambda s, c: (sweep(s, 0, True, False), c)[1], 0)

    def finish(s):
        def body(i, carry):
            a = jnp.where(i == 0, 1 - own_sub[s], own_sub[s])
            for j in range(heads_j):
                for g in range(group):
                    total = jnp.sum(l_ref[s, a, j, g], axis=1, keepdims=True)
                    o = (acc[s, a, j, g] / total).astype(jnp.bfloat16)
                    col = (j * group + g) * head_dim
                    ostage[1 - i, s, :, col:col + head_dim] = o
            return carry

        lax.fori_loop(0, 2, body, 0)

    def back(s):
        return pltpu.make_async_remote_copy(
            src_ref=ostage.at[1, s], dst_ref=orecv.at[s], send_sem=pair_send.at[4 + s], recv_sem=pair_recv.at[4 + s],
            device_id=partner, device_id_type=pl.DeviceIdType.MESH)

    def low_done():
        finish(0)
        back(0).start()

    def come(*which):
        def run():
            for side, slot in which:
                arrive(side, slot)
        return run

    def far_events():
        for s in range(2):
            event(s, far)
        for s in range(2):
            event(s, near, lambda s=s: col_of(s) == 0)

    def nothing():
        return None

    order = [
        (0, row, 0, nothing), (1, row, 1, nothing),
        (0, near, 0, far_events), (1, near, 0, nothing), (0, far, 0, nothing), (1, far, 1, nothing),
        (1, 2, 0, lambda: event(1, 2)), (0, 8, 0, come((0, 8))), (0, 2, 0, lambda: event(0, 2)),
        (1, row, 2, nothing), (1, far, 2, nothing),
        (0, 5, 0, come((0, 5))), (1, 5, 0, come((1, 5))), (0, 7, 0, come((0, 7))), (1, 8, 0, come((1, 8))),
        (0, 6, 0, come((0, 6))), (1, 7, 0, lambda: (low_done(), arrive(1, 7))), (1, 6, 0, come((1, 6))),
    ]

    def visit(i, carry):
        side = jnp.int32(0)
        slot = jnp.int32(0)
        kind = jnp.int32(0)
        for n, (s, d, when, prepare) in enumerate(order):
            side = jnp.where(i == n, s, side)
            slot = jnp.where(i == n, d, slot)
            kind = jnp.where(i == n, when, kind)
            if prepare is not nothing:
                @pl.when(i == n)
                def _():
                    prepare()

        late = plan.twin(jnp.where(side == 0, pairs[0], pairs[1]), slot) > near
        due = (kind == 0) | ((kind == 1) & jnp.logical_not(late)) | ((kind == 2) & late)

        @pl.when(due & (slot < plan.span))
        def _():
            sweep(side, slot)

        @pl.when(due & (slot == plan.span))
        def _():
            sweep(side, slot, True, True)
        return carry

    lax.fori_loop(0, len(order), visit, 0)
    finish(1)
    back(1).start()

    first_col = pl.multiple_of(core * half_cols, half_cols)
    other_col = pl.multiple_of(other * half_cols, half_cols)
    out_ref[:, :, pl.ds(first_col, half_cols)] = ostage[0]
    for s in range(2):
        back(s).wait_recv()
        out_ref[s, :, pl.ds(other_col, half_cols)] = orecv[s]
    for s in range(2):
        back(s).wait_send()
    for copy in pair_kv + [pair_x] + pair_turn:
        copy.wait_send()
    for spec in sent:
        copy, ok = describe(*spec)

        @pl.when(ok)
        def _():
            copy.wait_send()


def attend(plan, hidden, w_q, w_k, w_v, cos, sin):
    model_dim, heads, head_dim = w_q.shape
    kv_heads = w_k.shape[1]
    heads_j = kv_heads // 2
    chunk = hidden.shape[0] // 2
    group = heads // kv_heads
    bf16, f32 = jnp.bfloat16, jnp.float32
    slots = plan.span + 1
    half_heads = heads // 2
    depth = model_dim // 4
    vmem = pl.BlockSpec(memory_space=pltpu.VMEM)
    anywhere = pl.BlockSpec(memory_space=pl.ANY)
    return pl.pallas_call(
        functools.partial(attention_kernel, plan, kv_heads),
        out_shape=jax.ShapeDtypeStruct((2, chunk, heads * head_dim), bf16),
        in_specs=[anywhere, anywhere, anywhere, anywhere, vmem, vmem],
        out_specs=vmem,
        scratch_shapes=[
            pltpu.VMEM((2, 2, 2, heads_j, chunk, head_dim), bf16),
            pltpu.VMEM((2, 2, heads_j, group, chunk, head_dim), bf16),
            pltpu.VMEM((2, slots, 2, 2, heads_j, chunk, head_dim), bf16),
            pltpu.VMEM((2, 2, heads_j, group, chunk, head_dim), f32),
            pltpu.VMEM((2, 2, heads_j, group, chunk, head_dim), f32),
            pltpu.VMEM((2, 2, heads_j, group, chunk, head_dim), f32),
            pltpu.VMEM((2, 2, chunk, heads_j * group * head_dim), bf16),
            pltpu.VMEM((2, chunk, heads_j * group * head_dim), bf16),
            pltpu.VMEM((2, 2 * chunk, model_dim), bf16),
            pltpu.VMEM((2, 2, 2 * chunk, head_dim), f32),
            pltpu.VMEM((MIX, MIX), bf16),
            pltpu.VMEM((2, depth, half_heads, head_dim), bf16),
            pltpu.VMEM((model_dim, half_heads * head_dim), bf16),
            pltpu.SemaphoreType.DMA((4,)),
            pltpu.SemaphoreType.DMA,
            pltpu.SemaphoreType.DMA((2,)),
            pltpu.SemaphoreType.DMA((8,)),
            pltpu.SemaphoreType.DMA((8,)),
            pltpu.SemaphoreType.DMA((64,)),
            pltpu.SemaphoreType.DMA((2, slots)),
        ],
        compiler_params=pltpu.CompilerParams(collective_id=0, has_side_effects=True, vmem_limit_bytes=62 * 1024 * 1024),
        name='attend',
    )(hidden, w_k.reshape(-1, half_heads, head_dim), w_v.reshape(-1, half_heads, head_dim), w_q.reshape(model_dim, 2, half_heads, head_dim), cos, sin)


def solution(mesh):
    cp_size = mesh.shape['cp']
    plan = Plan(cp_size)

    def device_step(hidden, w_q, w_k, w_v, w_o):
        my_index = lax.axis_index('cp')
        chunk_len = hidden.shape[0] // 2
        model_dim = hidden.shape[1]
        heads, head_dim = w_q.shape[1], w_q.shape[2]
        chunk_ids = jnp.stack([my_index, 2 * cp_size - 1 - my_index])
        positions = (chunk_ids[:, None] * chunk_len + jnp.arange(chunk_len)[None, :]).reshape(2 * chunk_len)
        cos, sin = rotary_tables(positions, head_dim)
        attended = attend(plan, hidden, w_q, w_k, w_v, cos, sin)
        out_rows = jnp.dot(attended.reshape(2 * chunk_len, heads * head_dim), w_o.reshape(heads * head_dim, model_dim), preferred_element_type=jnp.float32)
        return out_rows.astype(jnp.bfloat16)

    return jax.shard_map(device_step, mesh=mesh, in_specs=(P(('dp', 'cp'), None), P(), P(), P(), P()), out_specs=P(('dp', 'cp'), None), check_vma=False)
```

```python
import functools
import math

import jax
import jax.numpy as jnp
from jax import lax
from jax.experimental import pallas as pl
from jax.experimental.pallas import tpu as pltpu
from jax.sharding import PartitionSpec as P

WINDOW = 4096
ROPE_BASE = 10000.0
NEG = -jnp.inf


def rotary_tables(positions, head_dim):
    half_dim = head_dim // 2
    inv_freq = 1.0 / (ROPE_BASE ** (jnp.arange(half_dim, dtype=jnp.float32) * (2.0 / head_dim)))
    angles = positions.astype(jnp.float32)[:, None] * inv_freq
    return jnp.cos(angles), jnp.sin(angles)


def spread(n_heads, size):
    per = size // n_heads
    to = lax.broadcasted_iota(jnp.int32, (size, size), 0)
    of = lax.broadcasted_iota(jnp.int32, (size, size), 1)
    return jnp.where((to % per) * n_heads + to // per == of, 1.0, 0.0).astype(jnp.bfloat16)


def by_head(mix, rows_ref, start, dst_ref, n_heads, base, col):
    size = mix.shape[0]
    per = size // n_heads
    head_dim = rows_ref.shape[2]
    first = pl.multiple_of(start // rows_ref.shape[1], 2 * size // rows_ref.shape[1])
    pair = rows_ref[pl.ds(first, 2 * size // rows_ref.shape[1])].reshape(2 * size, head_dim)
    wide = jnp.concatenate([pair[:size], pair[size:]], axis=1)
    out = jnp.dot(mix, wide, preferred_element_type=jnp.float32).astype(jnp.bfloat16)
    at = base + pl.multiple_of(start // n_heads, 2 * per)
    for b in range(2):
        for h in range(n_heads):
            cols = pl.ds(pl.multiple_of(col + h * head_dim, head_dim), head_dim)
            dst_ref[pl.ds(pl.multiple_of(at + b * per, per), per), cols] = out[h * per:(h + 1) * per, b * head_dim:(b + 1) * head_dim]


MIX = 256


class Plan:
    def __init__(self, cp_size):
        self.chips = cp_size // 2
        self.row = math.isqrt(self.chips)
        self.span = 2 * self.row

    def pair(self, chip, side):
        return jnp.where(side == 0, chip, 2 * self.chips - 1 - chip)

    def chip_of(self, pair):
        return jnp.where(pair < self.chips, pair, 2 * self.chips - 1 - pair)

    def side_of(self, pair):
        return jnp.where(pair < self.chips, 0, 1)

    def twin(self, pair, slot):
        same = 2 * self.chip_of(pair) + slot - (2 * self.chips - 1)
        return jnp.where(pair < self.chips, -1, same)


def attention_kernel(plan, kv_heads, x_hbm, wk_ref, wv_ref, wq_ref, cos_in, sin_in, out_ref, kv_ref, qbuf, kvbuf, acc, m_ref, l_ref,
                     ostage, orecv, x_ref, turns, mix, wraw, wsort, loc_sem, x_sem, w_sem, pair_send, pair_recv, send_sem, recv_sem):
    me = lax.axis_index('cp')
    chip = me // 2
    core = lax.rem(me, 2)
    other = 1 - core
    row = plan.row
    x = lax.rem(chip, row)
    y = chip // row
    n_row = plan.chips // row
    chunk = qbuf.shape[4]
    heads_j = qbuf.shape[2]
    group = qbuf.shape[3]
    head_dim = qbuf.shape[5]
    half_cols = heads_j * group * head_dim

    def device(target_chip, target_core):
        return {'cp': target_chip * 2 + target_core}

    barrier = pltpu.get_barrier_semaphore()
    pl.semaphore_signal(barrier, inc=1, device_id=device(chip, other), device_id_type=pl.DeviceIdType.MESH)
    for step in range(1, row):
        mate = y * row + lax.rem(x + step, row)
        pl.semaphore_signal(barrier, inc=1, device_id=device(mate, core), device_id_type=pl.DeviceIdType.MESH)
    for dy in (-1, 1):
        @pl.when((y + dy >= 0) & (y + dy < n_row))
        def _():
            pl.semaphore_signal(barrier, inc=1, device_id=device(chip + dy * row, core), device_id_type=pl.DeviceIdType.MESH)

    partner = device(chip, other)
    pairs = [plan.pair(chip, s) for s in range(2)]
    own_sub = [core, other]

    n_heads = heads_j * group
    depth = wraw.shape[1]
    n_kv = wk_ref.shape[0] // depth
    n_q = wq_ref.shape[0] // depth
    load_x = pltpu.make_async_copy(x_hbm, x_ref.at[0], x_sem)

    def fetch(block, part):
        at = pl.ds(pl.multiple_of(block * depth, depth), depth)
        slot = lax.rem(block, 2)
        src = (wk_ref.at[at], wv_ref.at[at], wq_ref.at[at, core] if part == 2 else None)[part]
        return pltpu.make_async_copy(src, wraw.at[slot], w_sem.at[slot])

    fetch(0, 0).start()
    load_x.start()

    turns[0, 0] = jnp.concatenate([cos_in[...], cos_in[...]], axis=1)
    turns[0, 1] = jnp.concatenate([-sin_in[...], sin_in[...]], axis=1)
    acc[...] = jnp.zeros_like(acc)
    l_ref[...] = jnp.zeros_like(l_ref)
    m_ref[...] = jnp.full_like(m_ref, NEG)

    mix[...] = spread(kv_heads, MIX)
    width = kv_heads * head_dim

    def sort(part, blocks, heads, follow):
        def step(block, carry):
            fetch(block, part).wait()

            @pl.when(block + 1 < blocks)
            def _():
                fetch(block + 1, part).start()

            @pl.when(block + 1 == blocks)
            def _():
                follow()

            raw = wraw.at[lax.rem(block, 2)]
            rows = depth * raw.shape[1] // heads
            base = pl.multiple_of(block * rows, rows)

            def arrange(i, c):
                by_head(mix[...], raw, pl.multiple_of(i * (2 * MIX), 2 * MIX), wsort, heads, base, width if part == 1 else 0)
                return c

            lax.fori_loop(0, depth * raw.shape[1] // (2 * MIX), arrange, 0, unroll=8)
            return carry

        lax.fori_loop(0, blocks, step, 0)

    sort(0, n_kv, kv_heads, lambda: fetch(0, 1).start())
    pl.semaphore_wait(barrier, row + jnp.where(y > 0, 1, 0) + jnp.where(y < n_row - 1, 1, 0))
    pair_x = pltpu.make_async_remote_copy(
        src_ref=x_hbm, dst_ref=x_ref.at[1], send_sem=pair_send.at[2], recv_sem=pair_recv.at[2],
        device_id=partner, device_id_type=pl.DeviceIdType.MESH)
    pair_x.start()
    sort(1, n_kv, kv_heads, lambda: fetch(0, 2).start())
    load_x.wait()
    wide = 2

    def project_kv(i, carry):
        first = lax.rem(i, kv_heads // wide)
        is_key = i < kv_heads // wide
        cols = pl.ds(pl.multiple_of(i * wide * head_dim, wide * head_dim), wide * head_dim)
        part = jnp.dot(x_ref[0], wsort[:, cols], preferred_element_type=jnp.float32)
        for s in range(2):
            rows = slice(s * chunk, (s + 1) * chunk)
            for h in range(wide):
                plain = part[rows, h * head_dim:(h + 1) * head_dim].astype(jnp.bfloat16).astype(jnp.float32)
                turned = plain * turns[0, 0, rows] + pltpu.roll(plain, head_dim // 2, 1) * turns[0, 1, rows]
                kv_ref[first, s, jnp.where(is_key, 0, 1), h] = jnp.where(is_key, turned, plain).astype(jnp.bfloat16)
        return carry

    lax.fori_loop(0, 2 * kv_heads // wide, project_kv, 0)

    pair_kv = []
    local = []
    for s in range(2):
        pair_kv.append(pltpu.make_async_remote_copy(
            src_ref=kv_ref.at[other, s], dst_ref=kvbuf.at[s, 0, own_sub[s]], send_sem=pair_send.at[s],
            recv_sem=pair_recv.at[s], device_id=partner, device_id_type=pl.DeviceIdType.MESH))
        local.append(pltpu.make_async_copy(kv_ref.at[core, s], kvbuf.at[s, 0, own_sub[s]], loc_sem.at[s]))
    for copy in pair_kv + local:
        copy.start()
    pair_turn = []
    for t in range(2):
        pair_turn.append(pltpu.make_async_remote_copy(
            src_ref=turns.at[0, t], dst_ref=turns.at[1, t], send_sem=pair_send.at[6 + t], recv_sem=pair_recv.at[6 + t],
            device_id=partner, device_id_type=pl.DeviceIdType.MESH))
        pair_turn[-1].start()

    def held(side, slot):
        twin = plan.twin(pairs[side], slot)
        return (jnp.where(twin >= 0, 0, side), jnp.where(twin >= 0, twin, slot))

    sent = []

    def along(side, step):
        col = lax.rem(pairs[side], row)
        return lax.rem(col + step, row) - col

    def describe(index, side, slot, where, cond):
        delta = where()
        node = pairs[side] + delta
        goal = slot + delta
        ok = (node < 2 * plan.chips) & (pairs[side] - slot >= 0) & (plan.twin(node, goal) < 0) & cond()
        held_side, held_slot = held(side, slot)
        copy = pltpu.make_async_remote_copy(
            src_ref=kvbuf.at[held_side, held_slot], dst_ref=kvbuf.at[plan.side_of(node), goal],
            send_sem=send_sem.at[index], recv_sem=recv_sem.at[plan.side_of(node), goal],
            device_id=device(plan.chip_of(node), core), device_id_type=pl.DeviceIdType.MESH)
        return copy, ok

    def send(side, slot, where, cond):
        spec = (len(sent), side, slot, where, cond)
        sent.append(spec)
        copy, ok = describe(*spec)

        @pl.when(ok)
        def _():
            copy.start()

    def arrive(side, slot, extra=True):
        ok = (pairs[side] - slot >= 0) & (plan.twin(pairs[side], slot) < 0) & extra

        @pl.when(ok)
        def _():
            buf = kvbuf.at[side, slot]
            pltpu.make_async_remote_copy(
                src_ref=buf, dst_ref=buf, send_sem=send_sem.at[0], recv_sem=recv_sem.at[side, slot],
                device_id=partner, device_id_type=pl.DeviceIdType.MESH).wait_recv()

    def always():
        return pairs[0] >= 0

    def down():
        return row

    for copy in pair_kv:
        copy.wait_recv()
    for copy in local:
        copy.wait()
    near, far = 1, row - 1

    def col_of(side):
        return lax.rem(pairs[side], row)

    def inner(side):
        return (col_of(side) > 0) & (col_of(side) < row - 1)

    def launch(side, slot, cond):
        send(side, slot, down, cond)
        if slot == 0 or slot == row:
            for step in (1, row - 1):
                where = functools.partial(along, side, step)
                send(side, slot, where, lambda w=where: cond() & ((w() > 0) if slot == 0 else (w() < 0)))
        elif slot == near:
            send(side, slot, lambda: 1, lambda: cond() & inner(side))
        elif slot == far:
            send(side, slot, lambda: -1, lambda: cond() & inner(side))

    def echo(slot, cond=lambda: pairs[0] >= 0):
        def as_high(d):
            return plan.twin(pairs[1], d) == slot
        for d in range(1, row + 1):
            if (d - slot) % 2 == 1 and d > slot:
                send(1, d, down, lambda d=d: as_high(d) & cond())

    def event(side, slot, cond=always):
        arrive(side, slot, cond())
        if side == 0:
            launch(0, slot, cond)
            echo(slot, cond)
        else:
            launch(1, slot, lambda: cond() & (plan.twin(pairs[1], slot) < 0))

    launch(0, 0, always)
    launch(1, 0, always)
    echo(0)

    mix[...] = spread(n_heads, MIX)
    sort(2, n_q, n_heads, lambda: None)
    per_rows = n_heads // wide

    def project(i, carry):
        whose = i // per_rows
        first = lax.rem(i, per_rows) * wide

        @pl.when(i == per_rows)
        def _():
            pair_x.wait_recv()
            for copy in pair_turn:
                copy.wait_recv()

        cols = pl.ds(pl.multiple_of(first * head_dim, wide * head_dim), wide * head_dim)
        part = jnp.dot(x_ref[whose], wsort[:, cols], preferred_element_type=jnp.float32)
        for s in range(2):
            rows = slice(s * chunk, (s + 1) * chunk)
            sub = jnp.where(whose == 0, own_sub[s], 1 - own_sub[s])
            for h in range(wide):
                q = part[rows, h * head_dim:(h + 1) * head_dim].astype(jnp.bfloat16).astype(jnp.float32)
                q = q * turns[whose, 0, rows] + pltpu.roll(q, head_dim // 2, 1) * turns[whose, 1, rows]
                qbuf[s, sub, first // group, lax.rem(first, group) + h] = (q * head_dim ** -0.5).astype(jnp.bfloat16)

        @pl.when(i == 2 * per_rows - 2)
        def _():
            event(0, row)
            event(1, row)
        return carry

    lax.fori_loop(0, 2 * per_rows, project, 0)

    def block(side, slot_side, slot, j, subs, masked, edge):
        k = kvbuf[slot_side, slot, :, 0, j].reshape(2 * chunk, head_dim)
        v = kvbuf[slot_side, slot, :, 1, j].reshape(2 * chunk, head_dim)
        tiles = [(a, g) for a in subs for g in range(group)]

        def score(t):
            a, g = tiles[t]
            return lax.dot_general(qbuf[side, a, j, g], k, (((1,), (1,)), ((), ())), preferred_element_type=jnp.float32)

        def update(t, s):
            a, g = tiles[t]
            if masked:
                rows = lax.broadcasted_iota(jnp.int32, (chunk, 2 * chunk), 0) + a * chunk
                cols = lax.broadcasted_iota(jnp.int32, (chunk, 2 * chunk), 1)
                s = jnp.where((cols > rows) if edge else (cols <= rows), s, NEG)
            m_old = m_ref[side, a, j, g]
            m_new = jnp.maximum(m_old, jnp.max(s, axis=1, keepdims=True))
            alpha = jnp.exp(m_old - m_new)
            e = jnp.exp(s - jnp.concatenate([m_new] * (2 * chunk // m_new.shape[1]), axis=1))
            part = e[:, :head_dim]
            for b in range(1, 2 * chunk // head_dim):
                part = part + e[:, b * head_dim:(b + 1) * head_dim]
            m_ref[side, a, j, g] = m_new
            l_ref[side, a, j, g] = l_ref[side, a, j, g] * alpha + part
            acc[side, a, j, g] = acc[side, a, j, g] * alpha + jnp.dot(e.astype(jnp.bfloat16), v, preferred_element_type=jnp.float32)

        ahead = 2
        scores = [score(t) for t in range(ahead)]
        for t in range(len(tiles)):
            if t + ahead < len(tiles):
                scores.append(score(t + ahead))
            update(t, scores[t])

    def sweep(side, slot, masked=False, edge=False):
        slot_side, at = held(side, slot) if isinstance(side, int) else (
            jnp.where(plan.twin(jnp.where(side == 0, pairs[0], pairs[1]), slot) >= 0, 0, side),
            jnp.where(plan.twin(jnp.where(side == 0, pairs[0], pairs[1]), slot) >= 0,
                      plan.twin(jnp.where(side == 0, pairs[0], pairs[1]), slot), slot))
        mine = jnp.where(side == 0, pairs[0], pairs[1])

        @pl.when(mine - slot >= 0)
        def _():
            def body(i, carry):
                block(side, slot_side, at, i, (0, 1), masked, edge)
                return carry
            lax.fori_loop(0, heads_j, body, 0)

    for s in range(2):
        event(s, near, lambda s=s: col_of(s) > 0)
    lax.fori_loop(0, 2, lambda s, c: (sweep(s, 0, True, False), c)[1], 0)

    def finish(s):
        def body(i, carry):
            a = jnp.where(i == 0, 1 - own_sub[s], own_sub[s])
            for j in range(heads_j):
                for g in range(group):
                    total = jnp.sum(l_ref[s, a, j, g], axis=1, keepdims=True)
                    o = (acc[s, a, j, g] / total).astype(jnp.bfloat16)
                    col = (j * group + g) * head_dim
                    ostage[1 - i, s, :, col:col + head_dim] = o
            return carry

        lax.fori_loop(0, 2, body, 0)

    def back(s):
        return pltpu.make_async_remote_copy(
            src_ref=ostage.at[1, s], dst_ref=orecv.at[s], send_sem=pair_send.at[4 + s], recv_sem=pair_recv.at[4 + s],
            device_id=partner, device_id_type=pl.DeviceIdType.MESH)

    def low_done():
        finish(0)
        back(0).start()

    def come(*which):
        def run():
            for side, slot in which:
                arrive(side, slot)
        return run

    def far_events():
        arrive(0, plan.span)
        event(1, far)
        event(0, near, lambda: col_of(0) == 0)
        event(0, far)

    def last_events():
        arrive(1, plan.span)
        event(0, 2)
        arrive(0, 7)

    def nothing():
        return None

    order = [
        (0, row, 0, nothing), (1, row, 1, nothing), (1, near, 0, lambda: event(1, near, lambda: col_of(1) == 0)),
        (0, 8, 0, far_events), (1, far, 1, nothing), (0, far, 0, nothing), (0, near, 0, nothing),
        (0, 5, 0, come((0, 5))), (1, 5, 1, come((1, 5))), (1, 2, 0, lambda: event(1, 2)),
        (1, 8, 0, last_events), (0, 7, 0, nothing), (0, 2, 0, nothing),
        (1, row, 2, nothing), (1, far, 2, nothing), (1, 5, 2, nothing),
        (0, 6, 0, come((0, 6), (1, 7))), (1, 7, 0, low_done), (1, 6, 0, come((1, 6))),
    ]

    def visit(i, carry):
        side = jnp.int32(0)
        slot = jnp.int32(0)
        kind = jnp.int32(0)
        for n, (s, d, when, prepare) in enumerate(order):
            side = jnp.where(i == n, s, side)
            slot = jnp.where(i == n, d, slot)
            kind = jnp.where(i == n, when, kind)
            if prepare is not nothing:
                @pl.when(i == n)
                def _():
                    prepare()

        late = plan.twin(jnp.where(side == 0, pairs[0], pairs[1]), slot) > near
        due = (kind == 0) | ((kind == 1) & jnp.logical_not(late)) | ((kind == 2) & late)

        @pl.when(due & (slot < plan.span))
        def _():
            sweep(side, slot)

        @pl.when(due & (slot == plan.span))
        def _():
            sweep(side, slot, True, True)
        return carry

    lax.fori_loop(0, len(order), visit, 0)
    finish(1)
    back(1).start()

    first_col = pl.multiple_of(core * half_cols, half_cols)
    other_col = pl.multiple_of(other * half_cols, half_cols)
    out_ref[:, :, pl.ds(first_col, half_cols)] = ostage[0]
    for s in range(2):
        back(s).wait_recv()
        out_ref[s, :, pl.ds(other_col, half_cols)] = orecv[s]
    for s in range(2):
        back(s).wait_send()
    for copy in pair_kv + [pair_x] + pair_turn:
        copy.wait_send()
    for spec in sent:
        copy, ok = describe(*spec)

        @pl.when(ok)
        def _():
            copy.wait_send()


def attend(plan, hidden, w_q, w_k, w_v, cos, sin):
    model_dim, heads, head_dim = w_q.shape
    kv_heads = w_k.shape[1]
    heads_j = kv_heads // 2
    chunk = hidden.shape[0] // 2
    group = heads // kv_heads
    bf16, f32 = jnp.bfloat16, jnp.float32
    slots = plan.span + 1
    half_heads = heads // 2
    depth = model_dim // 4
    vmem = pl.BlockSpec(memory_space=pltpu.VMEM)
    anywhere = pl.BlockSpec(memory_space=pl.ANY)
    return pl.pallas_call(
        functools.partial(attention_kernel, plan, kv_heads),
        out_shape=jax.ShapeDtypeStruct((2, chunk, heads * head_dim), bf16),
        in_specs=[anywhere, anywhere, anywhere, anywhere, vmem, vmem],
        out_specs=vmem,
        scratch_shapes=[
            pltpu.VMEM((2, 2, 2, heads_j, chunk, head_dim), bf16),
            pltpu.VMEM((2, 2, heads_j, group, chunk, head_dim), bf16),
            pltpu.VMEM((2, slots, 2, 2, heads_j, chunk, head_dim), bf16),
            pltpu.VMEM((2, 2, heads_j, group, chunk, head_dim), f32),
            pltpu.VMEM((2, 2, heads_j, group, chunk, head_dim), f32),
            pltpu.VMEM((2, 2, heads_j, group, chunk, head_dim), f32),
            pltpu.VMEM((2, 2, chunk, heads_j * group * head_dim), bf16),
            pltpu.VMEM((2, chunk, heads_j * group * head_dim), bf16),
            pltpu.VMEM((2, 2 * chunk, model_dim), bf16),
            pltpu.VMEM((2, 2, 2 * chunk, head_dim), f32),
            pltpu.VMEM((MIX, MIX), bf16),
            pltpu.VMEM((2, depth, half_heads, head_dim), bf16),
            pltpu.VMEM((model_dim, half_heads * head_dim), bf16),
            pltpu.SemaphoreType.DMA((2,)),
            pltpu.SemaphoreType.DMA,
            pltpu.SemaphoreType.DMA((2,)),
            pltpu.SemaphoreType.DMA((8,)),
            pltpu.SemaphoreType.DMA((8,)),
            pltpu.SemaphoreType.DMA((64,)),
            pltpu.SemaphoreType.DMA((2, slots)),
        ],
        compiler_params=pltpu.CompilerParams(collective_id=0, has_side_effects=True, vmem_limit_bytes=62 * 1024 * 1024),
        name='attend',
    )(hidden, w_k.reshape(-1, half_heads, head_dim), w_v.reshape(-1, half_heads, head_dim), w_q.reshape(model_dim, 2, half_heads, head_dim), cos, sin)


def solution(mesh):
    cp_size = mesh.shape['cp']
    plan = Plan(cp_size)

    def device_step(hidden, w_q, w_k, w_v, w_o):
        my_index = lax.axis_index('cp')
        chunk_len = hidden.shape[0] // 2
        model_dim = hidden.shape[1]
        heads, head_dim = w_q.shape[1], w_q.shape[2]
        chunk_ids = jnp.stack([my_index, 2 * cp_size - 1 - my_index])
        positions = (chunk_ids[:, None] * chunk_len + jnp.arange(chunk_len)[None, :]).reshape(2 * chunk_len)
        cos, sin = rotary_tables(positions, head_dim)
        attended = attend(plan, hidden, w_q, w_k, w_v, cos, sin)
        out_rows = jnp.dot(attended.reshape(2 * chunk_len, heads * head_dim), w_o.reshape(heads * head_dim, model_dim), preferred_element_type=jnp.float32)
        return out_rows.astype(jnp.bfloat16)

    return jax.shard_map(device_step, mesh=mesh, in_specs=(P(('dp', 'cp'), None), P(), P(), P(), P()), out_specs=P(('dp', 'cp'), None), check_vma=False)
```

```python
import functools
import math

import jax
import jax.numpy as jnp
from jax import lax
from jax.experimental import pallas as pl
from jax.experimental.pallas import tpu as pltpu
from jax.sharding import PartitionSpec as P

WINDOW = 4096
ROPE_BASE = 10000.0
NEG = -jnp.inf


def rotary_tables(positions, head_dim):
    half_dim = head_dim // 2
    inv_freq = 1.0 / (ROPE_BASE ** (jnp.arange(half_dim, dtype=jnp.float32) * (2.0 / head_dim)))
    angles = positions.astype(jnp.float32)[:, None] * inv_freq
    return jnp.cos(angles), jnp.sin(angles)


def spread(n_heads, size):
    per = size // n_heads
    to = lax.broadcasted_iota(jnp.int32, (size, size), 0)
    of = lax.broadcasted_iota(jnp.int32, (size, size), 1)
    return jnp.where((to % per) * n_heads + to // per == of, 1.0, 0.0).astype(jnp.bfloat16)


def by_head(mix, rows_ref, start, dst_ref, n_heads, base, col):
    size = mix.shape[0]
    per = size // n_heads
    head_dim = rows_ref.shape[2]
    first = pl.multiple_of(start // rows_ref.shape[1], 2 * size // rows_ref.shape[1])
    pair = rows_ref[pl.ds(first, 2 * size // rows_ref.shape[1])].reshape(2 * size, head_dim)
    wide = jnp.concatenate([pair[:size], pair[size:]], axis=1)
    out = jnp.dot(mix, wide, preferred_element_type=jnp.float32).astype(jnp.bfloat16)
    at = base + pl.multiple_of(start // n_heads, 2 * per)
    for b in range(2):
        for h in range(n_heads):
            cols = pl.ds(pl.multiple_of(col + h * head_dim, head_dim), head_dim)
            dst_ref[pl.ds(pl.multiple_of(at + b * per, per), per), cols] = out[h * per:(h + 1) * per, b * head_dim:(b + 1) * head_dim]


MIX = 256


class Plan:
    def __init__(self, cp_size):
        self.chips = cp_size // 2
        self.row = math.isqrt(self.chips)
        self.span = 2 * self.row

    def pair(self, chip, side):
        return jnp.where(side == 0, chip, 2 * self.chips - 1 - chip)

    def chip_of(self, pair):
        return jnp.where(pair < self.chips, pair, 2 * self.chips - 1 - pair)

    def side_of(self, pair):
        return jnp.where(pair < self.chips, 0, 1)

    def twin(self, pair, slot):
        same = 2 * self.chip_of(pair) + slot - (2 * self.chips - 1)
        return jnp.where(pair < self.chips, -1, same)


def attention_kernel(plan, kv_heads, x_hbm, wk_ref, wv_ref, wq_ref, cos_in, sin_in, out_ref, kv_ref, qbuf, kvbuf, acc, m_ref, l_ref,
                     ostage, orecv, x_ref, turns, mix, wraw, wsort, loc_sem, x_sem, w_sem, pair_send, pair_recv, send_sem, recv_sem):
    me = lax.axis_index('cp')
    chip = me // 2
    core = lax.rem(me, 2)
    other = 1 - core
    row = plan.row
    x = lax.rem(chip, row)
    y = chip // row
    n_row = plan.chips // row
    chunk = qbuf.shape[4]
    heads_j = qbuf.shape[2]
    group = qbuf.shape[3]
    head_dim = qbuf.shape[5]
    half_cols = heads_j * group * head_dim

    def device(target_chip, target_core):
        return {'cp': target_chip * 2 + target_core}

    barrier = pltpu.get_barrier_semaphore()
    pl.semaphore_signal(barrier, inc=1, device_id=device(chip, other), device_id_type=pl.DeviceIdType.MESH)
    for step in range(1, row):
        mate = y * row + lax.rem(x + step, row)
        pl.semaphore_signal(barrier, inc=1, device_id=device(mate, core), device_id_type=pl.DeviceIdType.MESH)
    for dy in (-1, 1):
        @pl.when((y + dy >= 0) & (y + dy < n_row))
        def _():
            pl.semaphore_signal(barrier, inc=1, device_id=device(chip + dy * row, core), device_id_type=pl.DeviceIdType.MESH)

    partner = device(chip, other)
    pairs = [plan.pair(chip, s) for s in range(2)]
    own_sub = [core, other]

    n_heads = heads_j * group
    depth = wraw.shape[1]
    n_kv = wk_ref.shape[0] // depth
    n_q = wq_ref.shape[0] // depth
    load_x = pltpu.make_async_copy(x_hbm, x_ref.at[0], x_sem)

    def fetch(block, part):
        at = pl.ds(pl.multiple_of(block * depth, depth), depth)
        slot = lax.rem(block, 2)
        src = (wk_ref.at[at], wv_ref.at[at], wq_ref.at[at, core] if part == 2 else None)[part]
        return pltpu.make_async_copy(src, wraw.at[slot], w_sem.at[slot])

    fetch(0, 0).start()
    load_x.start()

    turns[0, 0] = jnp.concatenate([cos_in[...], cos_in[...]], axis=1)
    turns[0, 1] = jnp.concatenate([-sin_in[...], sin_in[...]], axis=1)
    acc[...] = jnp.zeros_like(acc)
    l_ref[...] = jnp.zeros_like(l_ref)
    m_ref[...] = jnp.full_like(m_ref, NEG)

    mix[...] = spread(kv_heads, MIX)
    width = kv_heads * head_dim

    def sort(part, blocks, heads, follow):
        def step(block, carry):
            fetch(block, part).wait()

            @pl.when(block + 1 < blocks)
            def _():
                fetch(block + 1, part).start()

            @pl.when(block + 1 == blocks)
            def _():
                follow()

            raw = wraw.at[lax.rem(block, 2)]
            rows = depth * raw.shape[1] // heads
            base = pl.multiple_of(block * rows, rows)

            def arrange(i, c):
                by_head(mix[...], raw, pl.multiple_of(i * (2 * MIX), 2 * MIX), wsort, heads, base, width if part == 1 else 0)
                return c

            lax.fori_loop(0, depth * raw.shape[1] // (2 * MIX), arrange, 0, unroll=16)
            return carry

        lax.fori_loop(0, blocks, step, 0)

    sort(0, n_kv, kv_heads, lambda: fetch(0, 1).start())
    pl.semaphore_wait(barrier, row + jnp.where(y > 0, 1, 0) + jnp.where(y < n_row - 1, 1, 0))
    pair_x = pltpu.make_async_remote_copy(
        src_ref=x_hbm, dst_ref=x_ref.at[1], send_sem=pair_send.at[2], recv_sem=pair_recv.at[2],
        device_id=partner, device_id_type=pl.DeviceIdType.MESH)
    pair_x.start()
    sort(1, n_kv, kv_heads, lambda: fetch(0, 2).start())
    load_x.wait()
    wide = 2

    def project_kv(i, carry):
        first = lax.rem(i, kv_heads // wide)
        is_key = i < kv_heads // wide
        cols = pl.ds(pl.multiple_of(i * wide * head_dim, wide * head_dim), wide * head_dim)
        part = jnp.dot(x_ref[0], wsort[:, cols], preferred_element_type=jnp.float32)
        for s in range(2):
            rows = slice(s * chunk, (s + 1) * chunk)
            for h in range(wide):
                plain = part[rows, h * head_dim:(h + 1) * head_dim].astype(jnp.bfloat16).astype(jnp.float32)
                turned = plain * turns[0, 0, rows] + pltpu.roll(plain, head_dim // 2, 1) * turns[0, 1, rows]
                kv_ref[first, s, jnp.where(is_key, 0, 1), h] = jnp.where(is_key, turned, plain).astype(jnp.bfloat16)
        return carry

    lax.fori_loop(0, 2 * kv_heads // wide, project_kv, 0)

    pair_kv = []
    local = []
    for s in range(2):
        pair_kv.append(pltpu.make_async_remote_copy(
            src_ref=kv_ref.at[other, s], dst_ref=kvbuf.at[s, 0, own_sub[s]], send_sem=pair_send.at[s],
            recv_sem=pair_recv.at[s], device_id=partner, device_id_type=pl.DeviceIdType.MESH))
        local.append(pltpu.make_async_copy(kv_ref.at[core, s], kvbuf.at[s, 0, own_sub[s]], loc_sem.at[s]))
    for copy in pair_kv + local:
        copy.start()
    pair_turn = []
    for t in range(2):
        pair_turn.append(pltpu.make_async_remote_copy(
            src_ref=turns.at[0, t], dst_ref=turns.at[1, t], send_sem=pair_send.at[6 + t], recv_sem=pair_recv.at[6 + t],
            device_id=partner, device_id_type=pl.DeviceIdType.MESH))
        pair_turn[-1].start()

    def held(side, slot):
        twin = plan.twin(pairs[side], slot)
        return (jnp.where(twin >= 0, 0, side), jnp.where(twin >= 0, twin, slot))

    sent = []

    def along(side, step):
        col = lax.rem(pairs[side], row)
        return lax.rem(col + step, row) - col

    def describe(index, side, slot, where, cond):
        delta = where()
        node = pairs[side] + delta
        goal = slot + delta
        ok = (node < 2 * plan.chips) & (pairs[side] - slot >= 0) & (plan.twin(node, goal) < 0) & cond()
        held_side, held_slot = held(side, slot)
        copy = pltpu.make_async_remote_copy(
            src_ref=kvbuf.at[held_side, held_slot], dst_ref=kvbuf.at[plan.side_of(node), goal],
            send_sem=send_sem.at[index], recv_sem=recv_sem.at[plan.side_of(node), goal],
            device_id=device(plan.chip_of(node), core), device_id_type=pl.DeviceIdType.MESH)
        return copy, ok

    def send(side, slot, where, cond):
        spec = (len(sent), side, slot, where, cond)
        sent.append(spec)
        copy, ok = describe(*spec)

        @pl.when(ok)
        def _():
            copy.start()

    def arrive(side, slot, extra=True):
        ok = (pairs[side] - slot >= 0) & (plan.twin(pairs[side], slot) < 0) & extra

        @pl.when(ok)
        def _():
            buf = kvbuf.at[side, slot]
            pltpu.make_async_remote_copy(
                src_ref=buf, dst_ref=buf, send_sem=send_sem.at[0], recv_sem=recv_sem.at[side, slot],
                device_id=partner, device_id_type=pl.DeviceIdType.MESH).wait_recv()

    def always():
        return pairs[0] >= 0

    def down():
        return row

    for copy in pair_kv:
        copy.wait_recv()
    for copy in local:
        copy.wait()
    near, far = 1, row - 1

    def col_of(side):
        return lax.rem(pairs[side], row)

    def inner(side):
        return (col_of(side) > 0) & (col_of(side) < row - 1)

    def launch(side, slot, cond):
        send(side, slot, down, cond)
        if slot == 0 or slot == row:
            for step in (1, row - 1):
                where = functools.partial(along, side, step)
                send(side, slot, where, lambda w=where: cond() & ((w() > 0) if slot == 0 else (w() < 0)))
        elif slot == near:
            send(side, slot, lambda: 1, lambda: cond() & inner(side))
        elif slot == far:
            send(side, slot, lambda: -1, lambda: cond() & inner(side))

    def echo(slot, cond=lambda: pairs[0] >= 0):
        def as_high(d):
            return plan.twin(pairs[1], d) == slot
        for d in range(1, row + 1):
            if (d - slot) % 2 == 1 and d > slot:
                send(1, d, down, lambda d=d: as_high(d) & cond())

    def event(side, slot, cond=always):
        arrive(side, slot, cond())
        if side == 0:
            launch(0, slot, cond)
            echo(slot, cond)
        else:
            launch(1, slot, lambda: cond() & (plan.twin(pairs[1], slot) < 0))

    launch(0, 0, always)
    launch(1, 0, always)
    echo(0)

    mix[...] = spread(n_heads, MIX)
    sort(2, n_q, n_heads, lambda: None)
    per_rows = n_heads // wide

    def project(i, carry):
        whose = i // per_rows
        first = lax.rem(i, per_rows) * wide

        @pl.when(i == per_rows)
        def _():
            pair_x.wait_recv()
            for copy in pair_turn:
                copy.wait_recv()

        cols = pl.ds(pl.multiple_of(first * head_dim, wide * head_dim), wide * head_dim)
        part = jnp.dot(x_ref[whose], wsort[:, cols], preferred_element_type=jnp.float32)
        for s in range(2):
            rows = slice(s * chunk, (s + 1) * chunk)
            sub = jnp.where(whose == 0, own_sub[s], 1 - own_sub[s])
            for h in range(wide):
                q = part[rows, h * head_dim:(h + 1) * head_dim].astype(jnp.bfloat16).astype(jnp.float32)
                q = q * turns[whose, 0, rows] + pltpu.roll(q, head_dim // 2, 1) * turns[whose, 1, rows]
                qbuf[s, sub, first // group, lax.rem(first, group) + h] = (q * head_dim ** -0.5).astype(jnp.bfloat16)

        @pl.when(i == 2 * per_rows - 2)
        def _():
            event(0, row)
            event(1, row)
        return carry

    lax.fori_loop(0, 2 * per_rows, project, 0)

    def block(side, slot_side, slot, j, subs, masked, edge):
        k = kvbuf[slot_side, slot, :, 0, j].reshape(2 * chunk, head_dim)
        v = kvbuf[slot_side, slot, :, 1, j].reshape(2 * chunk, head_dim)
        tiles = list(subs)
        tall = group * chunk

        def score(t):
            return lax.dot_general(qbuf[side, tiles[t], j].reshape(tall, head_dim), k, (((1,), (1,)), ((), ())), preferred_element_type=jnp.float32)

        def update(t, s):
            a = tiles[t]
            if masked:
                rows = lax.broadcasted_iota(jnp.int32, (tall, 2 * chunk), 0) % chunk + a * chunk
                cols = lax.broadcasted_iota(jnp.int32, (tall, 2 * chunk), 1)
                s = jnp.where((cols > rows) if edge else (cols <= rows), s, NEG)
            m_old = m_ref[side, a, j].reshape(tall, head_dim)
            m_new = jnp.maximum(m_old, jnp.max(s, axis=1, keepdims=True))
            alpha = jnp.exp(m_old - m_new)
            e = jnp.exp(s - jnp.concatenate([m_new] * (2 * chunk // m_new.shape[1]), axis=1))
            part = e[:, :head_dim]
            for b in range(1, 2 * chunk // head_dim):
                part = part + e[:, b * head_dim:(b + 1) * head_dim]
            m_ref[side, a, j] = m_new.reshape(group, chunk, head_dim)
            l_ref[side, a, j] = (l_ref[side, a, j].reshape(tall, head_dim) * alpha + part).reshape(group, chunk, head_dim)
            total = acc[side, a, j].reshape(tall, head_dim) * alpha + jnp.dot(e.astype(jnp.bfloat16), v, preferred_element_type=jnp.float32)
            acc[side, a, j] = total.reshape(group, chunk, head_dim)

        ahead = 1
        scores = [score(t) for t in range(ahead)]
        for t in range(len(tiles)):
            if t + ahead < len(tiles):
                scores.append(score(t + ahead))
            update(t, scores[t])

    def sweep(side, slot, masked=False, edge=False):
        slot_side, at = held(side, slot) if isinstance(side, int) else (
            jnp.where(plan.twin(jnp.where(side == 0, pairs[0], pairs[1]), slot) >= 0, 0, side),
            jnp.where(plan.twin(jnp.where(side == 0, pairs[0], pairs[1]), slot) >= 0,
                      plan.twin(jnp.where(side == 0, pairs[0], pairs[1]), slot), slot))
        mine = jnp.where(side == 0, pairs[0], pairs[1])

        @pl.when(mine - slot >= 0)
        def _():
            def body(i, carry):
                block(side, slot_side, at, i, (0, 1), masked, edge)
                return carry
            lax.fori_loop(0, heads_j, body, 0)

    for s in range(2):
        event(s, near, lambda s=s: col_of(s) > 0)
    lax.fori_loop(0, 2, lambda s, c: (sweep(s, 0, True, False), c)[1], 0)

    def finish(s):
        def body(i, carry):
            a = jnp.where(i == 0, 1 - own_sub[s], own_sub[s])
            for j in range(heads_j):
                for g in range(group):
                    total = jnp.sum(l_ref[s, a, j, g], axis=1, keepdims=True)
                    o = (acc[s, a, j, g] / total).astype(jnp.bfloat16)
                    col = (j * group + g) * head_dim
                    ostage[1 - i, s, :, col:col + head_dim] = o
            return carry

        lax.fori_loop(0, 2, body, 0)

    def back(s):
        return pltpu.make_async_remote_copy(
            src_ref=ostage.at[1, s], dst_ref=orecv.at[s], send_sem=pair_send.at[4 + s], recv_sem=pair_recv.at[4 + s],
            device_id=partner, device_id_type=pl.DeviceIdType.MESH)

    def low_done():
        finish(0)
        back(0).start()

    def come(*which):
        def run():
            for side, slot in which:
                arrive(side, slot)
        return run

    def far_events():
        arrive(0, plan.span)
        event(1, far)
        event(0, near, lambda: col_of(0) == 0)
        event(0, far)

    def last_events():
        arrive(1, plan.span)
        event(0, 2)
        arrive(0, 7)

    def nothing():
        return None

    order = [
        (0, row, 0, nothing), (1, row, 1, nothing), (1, near, 0, lambda: event(1, near, lambda: col_of(1) == 0)),
        (0, 8, 0, far_events), (1, far, 1, nothing), (0, far, 0, nothing), (0, near, 0, nothing),
        (0, 5, 0, come((0, 5))), (1, 5, 1, come((1, 5))), (1, 2, 0, lambda: event(1, 2)),
        (1, 8, 0, last_events), (0, 7, 0, nothing), (0, 2, 0, nothing),
        (1, row, 2, nothing), (1, far, 2, nothing), (1, 5, 2, nothing),
        (0, 6, 0, come((0, 6), (1, 7))), (1, 7, 0, low_done), (1, 6, 0, come((1, 6))),
    ]

    def visit(i, carry):
        side = jnp.int32(0)
        slot = jnp.int32(0)
        kind = jnp.int32(0)
        for n, (s, d, when, prepare) in enumerate(order):
            side = jnp.where(i == n, s, side)
            slot = jnp.where(i == n, d, slot)
            kind = jnp.where(i == n, when, kind)
            if prepare is not nothing:
                @pl.when(i == n)
                def _():
                    prepare()

        late = plan.twin(jnp.where(side == 0, pairs[0], pairs[1]), slot) > near
        due = (kind == 0) | ((kind == 1) & jnp.logical_not(late)) | ((kind == 2) & late)

        @pl.when(due & (slot < plan.span))
        def _():
            sweep(side, slot)

        @pl.when(due & (slot == plan.span))
        def _():
            sweep(side, slot, True, True)
        return carry

    lax.fori_loop(0, len(order), visit, 0)
    finish(1)
    back(1).start()

    first_col = pl.multiple_of(core * half_cols, half_cols)
    other_col = pl.multiple_of(other * half_cols, half_cols)
    out_ref[:, :, pl.ds(first_col, half_cols)] = ostage[0]
    for s in range(2):
        back(s).wait_recv()
        out_ref[s, :, pl.ds(other_col, half_cols)] = orecv[s]
    for s in range(2):
        back(s).wait_send()
    for copy in pair_kv + [pair_x] + pair_turn:
        copy.wait_send()
    for spec in sent:
        copy, ok = describe(*spec)

        @pl.when(ok)
        def _():
            copy.wait_send()


def attend(plan, hidden, w_q, w_k, w_v, cos, sin):
    model_dim, heads, head_dim = w_q.shape
    kv_heads = w_k.shape[1]
    heads_j = kv_heads // 2
    chunk = hidden.shape[0] // 2
    group = heads // kv_heads
    bf16, f32 = jnp.bfloat16, jnp.float32
    slots = plan.span + 1
    half_heads = heads // 2
    depth = model_dim // 4
    vmem = pl.BlockSpec(memory_space=pltpu.VMEM)
    anywhere = pl.BlockSpec(memory_space=pl.ANY)
    return pl.pallas_call(
        functools.partial(attention_kernel, plan, kv_heads),
        out_shape=jax.ShapeDtypeStruct((2, chunk, heads * head_dim), bf16),
        in_specs=[anywhere, anywhere, anywhere, anywhere, vmem, vmem],
        out_specs=vmem,
        scratch_shapes=[
            pltpu.VMEM((2, 2, 2, heads_j, chunk, head_dim), bf16),
            pltpu.VMEM((2, 2, heads_j, group, chunk, head_dim), bf16),
            pltpu.VMEM((2, slots, 2, 2, heads_j, chunk, head_dim), bf16),
            pltpu.VMEM((2, 2, heads_j, group, chunk, head_dim), f32),
            pltpu.VMEM((2, 2, heads_j, group, chunk, head_dim), f32),
            pltpu.VMEM((2, 2, heads_j, group, chunk, head_dim), f32),
            pltpu.VMEM((2, 2, chunk, heads_j * group * head_dim), bf16),
            pltpu.VMEM((2, chunk, heads_j * group * head_dim), bf16),
            pltpu.VMEM((2, 2 * chunk, model_dim), bf16),
            pltpu.VMEM((2, 2, 2 * chunk, head_dim), f32),
            pltpu.VMEM((MIX, MIX), bf16),
            pltpu.VMEM((2, depth, half_heads, head_dim), bf16),
            pltpu.VMEM((model_dim, half_heads * head_dim), bf16),
            pltpu.SemaphoreType.DMA((2,)),
            pltpu.SemaphoreType.DMA,
            pltpu.SemaphoreType.DMA((2,)),
            pltpu.SemaphoreType.DMA((8,)),
            pltpu.SemaphoreType.DMA((8,)),
            pltpu.SemaphoreType.DMA((64,)),
            pltpu.SemaphoreType.DMA((2, slots)),
        ],
        compiler_params=pltpu.CompilerParams(collective_id=0, has_side_effects=True, vmem_limit_bytes=62 * 1024 * 1024),
        name='attend',
    )(hidden, w_k.reshape(-1, half_heads, head_dim), w_v.reshape(-1, half_heads, head_dim), w_q.reshape(model_dim, 2, half_heads, head_dim), cos, sin)


def solution(mesh):
    cp_size = mesh.shape['cp']
    plan = Plan(cp_size)

    def device_step(hidden, w_q, w_k, w_v, w_o):
        my_index = lax.axis_index('cp')
        chunk_len = hidden.shape[0] // 2
        model_dim = hidden.shape[1]
        heads, head_dim = w_q.shape[1], w_q.shape[2]
        chunk_ids = jnp.stack([my_index, 2 * cp_size - 1 - my_index])
        positions = (chunk_ids[:, None] * chunk_len + jnp.arange(chunk_len)[None, :]).reshape(2 * chunk_len)
        cos, sin = rotary_tables(positions, head_dim)
        attended = attend(plan, hidden, w_q, w_k, w_v, cos, sin)
        out_rows = jnp.dot(attended.reshape(2 * chunk_len, heads * head_dim), w_o.reshape(heads * head_dim, model_dim), preferred_element_type=jnp.float32)
        return out_rows.astype(jnp.bfloat16)

    return jax.shard_map(device_step, mesh=mesh, in_specs=(P(('dp', 'cp'), None), P(), P(), P(), P()), out_specs=P(('dp', 'cp'), None), check_vma=False)
```
